128 devices in a mesh: lon: 16 (over x, z_hi, core), lat: 8 (over y, z_lo).
Axes of the slice: x: 4, y: 4, z: 4 (z_hi: 2, z_lo: 2; z = z_hi * 2 + z_lo), core: 2. Of those that a mesh axis runs over, the one named last changes fastest.
Arguments:
- fields: bfloat16 [4, 2, 1024, 4096], P(None, None, 'lat', 'lon'), may hold values from -6 to 6
- shifts: int32 [2, 64], P(None, 'lat'), may hold values from 0 to 4095
- fractions: float32 [2, 1024, 4096], P(None, 'lat', 'lon'), may hold values from 0 to 1
- helm_coef: float32 [2], replicated, may hold values from 1 to 16
Outputs:
- fields_out: bfloat16 [4, 2, 1024, 4096], P(None, None, 'lat', 'lon')
The draws below stay inside these ranges and needn't reach their ends.
All inputs are finite; a program needn't handle non-finite values.
Results may differ from the reference program's by a relative error of at most 0.0044.
The reference program's roundings to bfloat16 on the way count: a program that leaves them out, or rounds other values in their place, can miss the bound.
Values may be sent and summed in bfloat16 or wider, within the bound.
A program may use at most 64 MiB of HBM per device.

```python
import math
import jax
import jax.numpy as jnp
from jax import lax

RB = 16
LEV = 2
FIELDS = 4
STEPS = 2
SWEEPS = 8
NLON = 4096
NLAT = 1024
NBLK = 64


def place_ends(values, rng, low, high):
    longest = values.shape.index(max(values.shape))
    spots = []
    for shift in (0, 1):
        where = [jax.random.randint(jax.random.fold_in(rng, axis), (), 0, length) for axis, length in enumerate(values.shape)]
        where[longest] = (where[longest] + shift) % values.shape[longest]
        spots.append(tuple(where))
    return values.at[spots[0]].set(low).at[spots[1]].set(high)


def level_of(key, extent, split, least, largest):
    def one(axis_at, blocks):
        draws = jax.random.uniform(jax.random.fold_in(jax.random.fold_in(key, 6), axis_at), (blocks,), jnp.float32, least / len(split), largest / len(split))
        return jnp.repeat(jnp.exp(draws), extent[axis_at] // blocks).reshape((-1,) + (1,) * (len(extent) - axis_at - 1))

    loudness = one(*split[0])
    for cut in split[1:]:
        loudness = loudness * one(*cut)
    return loudness


def centred(rng, extent, scale, limit, pieces=(), kind=jnp.bfloat16):
    values = jax.random.normal(rng, extent, jnp.float32) * scale
    if len(pieces) > 0:
        values = level_of(rng, extent, pieces, -0.22, 0.18) * values
    return jnp.clip(values, min=-limit, max=limit).astype(kind)


def setup_inputs(seed: int = 0) -> dict:
    key_list = jax.random.split(jax.random.key(seed), 5)
    fields = centred(key_list[0], (FIELDS, LEV, NLAT, NLON), 1.0, 6.0, ((2, 8), (3, 16)))
    shifts = place_ends(jax.random.randint(key_list[1], (STEPS, NBLK), 0, NLON), jax.random.fold_in(key_list[1], 1), 0, NLON - 1).astype(jnp.int32)
    fractions = jnp.clip(1.0 * jax.random.uniform(key_list[2], (STEPS, NLAT, NLON), jnp.float32) ** level_of(key_list[2], (STEPS, NLAT, NLON), ((1, 8), (2, 16)), -0.2, 0.2), 0.0, 1.0)
    helm_coef = jnp.clip(jnp.exp(jax.random.uniform(key_list[3], (LEV,), jnp.float32, math.log(1.0), math.log(16.0))), 1.0, 16.0)
    return dict(fields=fields, shifts=shifts, fractions=fractions, helm_coef=helm_coef)


TAU = 0.5


def cubic_weights(fraction):
    return (-fraction * (fraction - 1.0) * (fraction - 2.0) / 6.0,
            (fraction + 1.0) * (fraction - 1.0) * (fraction - 2.0) / 2.0,
            -(fraction + 1.0) * fraction * (fraction - 2.0) / 2.0,
            (fraction + 1.0) * fraction * (fraction - 1.0) / 6.0)


def advect(current, shift_row, frac_row):
    lon_total = current.shape[3]
    blocks = jnp.moveaxis(current.reshape(FIELDS, LEV, NBLK, RB, lon_total), 2, 0)
    block_fracs = frac_row.reshape(NBLK, RB, lon_total)

    def interp_block(block_item):
        block_rows, block_frac, block_shift = block_item
        doubled = jnp.concatenate([block_rows, block_rows], axis=3)
        node_weights = cubic_weights(block_frac)
        accumulated = jnp.zeros(block_rows.shape, jnp.float32)
        for node_index in range(4):
            offset = (block_shift - 1 + node_index) % lon_total
            start = ((lon_total - offset) % lon_total).astype(jnp.int32)
            sampled = lax.dynamic_slice_in_dim(doubled, start, lon_total, axis=3)
            accumulated = accumulated + node_weights[node_index] * sampled.astype(jnp.float32)
        return accumulated.astype(jnp.bfloat16)

    result = lax.map(interp_block, (blocks, block_fracs, shift_row))
    return jnp.moveaxis(result, 0, 2).reshape(current.shape)


def diff_lon(values_in):
    return 0.5 * (jnp.roll(values_in, -1, axis=2) - jnp.roll(values_in, 1, axis=2))


def diff_lat(values_in):
    padded = jnp.pad(values_in, ((0, 0), (1, 1), (0, 0)))
    return 0.5 * (padded[:, 2:, :] - padded[:, :-2, :])


def neighbour_sum(potential):
    padded = jnp.pad(potential, ((0, 0), (1, 1), (0, 0)))
    return (jnp.roll(potential, -1, axis=2) + jnp.roll(potential, 1, axis=2)) + (padded[:, 2:, :] + padded[:, :-2, :])


def reference(fields, shifts, fractions, helm_coef):
    coefficient = helm_coef[:, None, None]
    current = fields
    for step_index in range(STEPS):
        advected = advect(current, shifts[step_index], fractions[step_index])
        flux = advected.astype(jnp.float32)
        source = flux[0] - TAU * (diff_lon(flux[1]) + diff_lat(flux[2]))
        potential = source
        for sweep_index in range(SWEEPS):
            potential = (source + coefficient * neighbour_sum(potential)) / (1.0 + 4.0 * coefficient)
        east_wind = flux[1] - TAU * diff_lon(potential)
        north_wind = flux[2] - TAU * diff_lat(potential)
        current = jnp.stack([potential, east_wind, north_wind, flux[3]]).astype(jnp.bfloat16)
    return current
```

```python
import functools

import jax
import jax.numpy as jnp
from jax import lax
from jax.experimental import pallas as pl
from jax.experimental.pallas import tpu as pltpu
from jax.sharding import PartitionSpec as P

STEPS = 2
SWEEPS = 8
ROWS = 16
LANES = 128
GROUP = 8
F32 = jnp.float32
BF16 = jnp.bfloat16
MESH = pl.DeviceIdType.MESH


def place_of(lon):
    return 2 * (lon // 4) + lon % 2, (lon // 2) % 2


def lon_of(block, level):
    return 4 * (block // 2) + 2 * level + block % 2


def cubic_weights(a):
    am, ap, a2 = a - 1.0, a + 1.0, a - 2.0
    left, right = a * am, ap * a2
    return (
        left * a2 * (-1.0 / 6.0),
        right * am * 0.5,
        right * a * -0.5,
        ap * left * (1.0 / 6.0),
    )


def kernel(
    n_lon, n_lat, fields, shifts, fractions, helm, out,
    x, frac, field, adv, res, src, scaled, pot, down, up, above, below,
    in_send, in_recv, halo_send, halo_recv, out_send, out_recv,
):
    n_cols = n_lon * fields.shape[3]
    tile = fields.shape[3]
    n_chunks = n_cols // LANES
    n_blocks = fields.shape[2] // ROWS
    lon, lat = lax.axis_index("lon"), lax.axis_index("lat")
    block, level = place_of(lon)

    prev_block = lax.rem(block + n_blocks - 1, n_blocks)
    next_block = lax.rem(block + 1, n_blocks)
    lat_up = lax.rem(lat + n_lat - (block == 0).astype(jnp.int32), n_lat)
    lat_down = lax.rem(lat + (block == n_blocks - 1).astype(jnp.int32), n_lat)
    dev_up = {"lon": lon_of(prev_block, level), "lat": lat_up}
    dev_down = {"lon": lon_of(next_block, level), "lat": lat_down}
    row_block = lat * n_blocks + block
    has_above = row_block > 0
    has_below = row_block < n_lat * n_blocks - 1

    def rows_of(b):
        return pl.ds(pl.multiple_of(b * ROWS, ROWS), ROWS)

    def cols_of(p):
        return pl.ds(pl.multiple_of(p * tile, tile), tile)

    def chunk(k):
        return pl.ds(pl.multiple_of(k * LANES, LANES), LANES)

    barrier = pltpu.get_barrier_semaphore()

    def greet(j, _):
        peer = lax.rem(lon + j, n_lon)
        pl.semaphore_signal(barrier, inc=1, device_id={"lon": peer, "lat": lat}, device_id_type=MESH)
        return 0

    lax.fori_loop(1, n_lon, greet, 0)
    pl.semaphore_signal(barrier, inc=1, device_id=dev_up, device_id_type=MESH)
    pl.semaphore_signal(barrier, inc=1, device_id=dev_down, device_id_type=MESH)
    pl.semaphore_wait(barrier, n_lon + 1)

    def in_refs(part, to_block, to_level, from_lon):
        if part == 0:
            return (fields.at[0:3, to_level, rows_of(to_block), :], x.at[0:3, :, cols_of(from_lon)])
        if part == 2:
            return (fields.at[3, to_level, rows_of(to_block), :], x.at[3, :, cols_of(from_lon)])
        step = part // 2
        return (fractions.at[step, rows_of(to_block), :], frac.at[step, :, cols_of(from_lon)])

    def send_parts(parts):
        def turn(j, _):
            peer = lax.rem(lon + j, n_lon)
            to_block, to_level = place_of(peer)
            for part in parts:
                from_ref, to_ref = in_refs(part, to_block, to_level, lon)
                pltpu.make_async_remote_copy(
                    src_ref=from_ref,
                    dst_ref=to_ref,
                    send_sem=in_send.at[part],
                    recv_sem=in_recv.at[part],
                    device_id={"lon": peer, "lat": lat},
                    device_id_type=MESH,
                ).start()
            return 0

        lax.fori_loop(1, n_lon, turn, 0)
        for part in parts:
            from_ref, to_ref = in_refs(part, block, level, lon)
            pltpu.make_async_copy(from_ref, to_ref, in_recv.at[part]).start()

    def in_whole(part):
        return (x.at[0:3], frac.at[0], x.at[3], frac.at[1])[part]

    def wait_in(part):
        whole = in_whole(part)
        pltpu.make_async_copy(whole, whole, in_recv.at[part]).wait()

    def wait_in_sent(part):
        whole = in_whole(part)
        sent = whole.at[:, :, 0 : n_cols - tile] if part == 0 else whole.at[:, 0 : n_cols - tile]
        pltpu.make_async_copy(sent, sent, in_send.at[part]).wait()

    send_parts((0, 1))
    send_parts((2, 3))

    lane = lax.broadcasted_iota(jnp.int32, (ROWS, LANES), 1)
    row16 = lax.broadcasted_iota(jnp.int32, (ROWS, LANES), 0)
    lane32 = lax.broadcasted_iota(jnp.int32, (2 * ROWS, LANES), 1)
    row32 = lax.broadcasted_iota(jnp.int32, (2 * ROWS, LANES), 0)

    coef = jnp.full((2 * ROWS, LANES), helm[level], F32)
    inverse = 1.0 / (1.0 + 4.0 * coef)
    inside = ((row32 >= 8) | has_above) & ((row32 < 24) | has_below)
    weight = jnp.where(inside, coef * inverse, 0.0)

    def unpack(parts):
        def turn(g, _):
            for j in range(GROUP):
                k = g * GROUP + j
                for f in parts:
                    field[f, k] = x[f, :, chunk(k)].astype(F32)
            return 0

        lax.fori_loop(0, n_chunks // GROUP, turn, 0)

    def advect(step, sources, targets):
        shift = shifts[step, block]
        taps = []
        for d in (1, 0, -1, -2):
            total = lax.rem(shift + (n_cols - d), n_cols)
            taps.append((lax.div(total, LANES), lax.rem(total, LANES)))
        from_here = [lane >= part for _, part in taps]

        def rolled(f, k, tap):
            whole, part = taps[tap]
            at = lax.rem(k - whole + 2 * n_chunks, n_chunks)
            return pltpu.roll(field[f, at], part, 1)

        first = tuple(rolled(f, -1, tap) for f in sources for tap in range(4))

        def turn(k, before):
            w = cubic_weights(frac[step, :, chunk(k)])
            now = []
            for f, to in zip(sources, targets):
                total = None
                for tap in range(4):
                    here = rolled(f, k, tap)
                    value = jnp.where(from_here[tap], here, before[len(now)])
                    now.append(here)
                    total = w[tap] * value if total is None else total + w[tap] * value
                to(k, total.astype(BF16))
            return tuple(now)

        lax.fori_loop(0, n_chunks, turn, first, unroll=2)

    def around(g, load):
        base = g * GROUP
        vals = [load(lax.rem(base + j + n_chunks, n_chunks)) for j in range(-1, GROUP + 1)]
        return vals

    def east_west(vals, ln):
        east = [None] + [pltpu.roll(v, LANES - 1, 1) for v in vals[1:]]
        west = [pltpu.roll(v, 1, 1) for v in vals[:-1]]
        last, first = ln == LANES - 1, ln == 0
        return [
            (
                jnp.where(last, east[j + 1], east[j]),
                jnp.where(first, west[j - 1], west[j]),
            )
            for j in range(1, len(vals) - 1)
        ]

    def sources(step):
        def turn(g, _):
            wind = around(g, lambda k: adv[1, :, chunk(k)].astype(F32))
            for j, (e, w) in enumerate(east_west(wind, lane)):
                k = g * GROUP + j
                north = adv[2, :, chunk(k)].astype(F32)
                after = jnp.where(row16 == ROWS - 1, 0.0, pltpu.roll(north, ROWS - 1, 0))
                prior = jnp.where(row16 == 0, 0.0, pltpu.roll(north, 1, 0))
                own = adv[0, :, chunk(k)].astype(F32) - 0.25 * ((e - w) + (after - prior))
                src[ROWS : 2 * ROWS, chunk(k)] = own
                turned = pltpu.roll(north, 1, 0)
                down[step, :, chunk(k)] = jnp.where(row16 == 0, turned, own).astype(BF16)
                turned = pltpu.roll(north, ROWS - 1, 0)
                up[step, :, chunk(k)] = jnp.where(row16 == ROWS - 1, turned, own).astype(BF16)
            return 0

        lax.fori_loop(0, n_chunks // GROUP, turn, 0)

    def halo_copies(step):
        return (
            pltpu.make_async_remote_copy(
                src_ref=down.at[step],
                dst_ref=above.at[step],
                send_sem=halo_send.at[step, 0],
                recv_sem=halo_recv.at[step, 0],
                device_id=dev_down,
                device_id_type=MESH,
            ),
            pltpu.make_async_remote_copy(
                src_ref=up.at[step],
                dst_ref=below.at[step],
                send_sem=halo_send.at[step, 1],
                recv_sem=halo_recv.at[step, 1],
                device_id=dev_up,
                device_id_type=MESH,
            ),
        )

    def complete(step):
        def turn(g, _):
            for j in range(GROUP):
                k = g * GROUP + j
                north = adv[2, :, chunk(k)].astype(F32)
                own = src[ROWS : 2 * ROWS, chunk(k)]
                a = jnp.where(has_above, above[step, :, chunk(k)].astype(F32), 0.0)
                b = jnp.where(has_below, below[step, :, chunk(k)].astype(F32), 0.0)
                own = own + 0.25 * jnp.where(row16 == 0, a, 0.0)
                own = own - 0.25 * jnp.where(row16 == ROWS - 1, b, 0.0)
                to_a = jnp.where((row16 == ROWS - 1) & has_above, pltpu.roll(north, ROWS - 1, 0), 0.0)
                to_b = jnp.where((row16 == 0) & has_below, pltpu.roll(north, 1, 0), 0.0)
                src[0:ROWS, chunk(k)] = a - 0.25 * to_a
                src[ROWS : 2 * ROWS, chunk(k)] = own
                src[2 * ROWS : 3 * ROWS, chunk(k)] = b + 0.25 * to_b
            return 0

        lax.fori_loop(0, n_chunks // GROUP, turn, 0)

    def first_sweep():
        def turn(g, _):
            vals = around(g, lambda k: src[8:40, chunk(k)])
            for j, (e, w) in enumerate(east_west(vals, lane32)):
                k = g * GROUP + j
                column = src[:, chunk(k)]
                n = pltpu.roll(column, 1, 0)[8:40]
                s = pltpu.roll(column, 3 * ROWS - 1, 0)[8:40]
                fixed = vals[j + 1] * inverse
                scaled[:, chunk(k)] = fixed
                pot[0, :, chunk(k)] = fixed + weight * ((e + w) + (n + s))
            return 0

        lax.fori_loop(0, n_chunks // GROUP, turn, 0)

    def later_sweeps():
        def sweep(i, _):
            now, then = lax.rem(i, 2), lax.rem(i + 1, 2)

            def turn(g, _):
                vals = around(g, lambda k: pot[now, :, chunk(k)])
                for j, (e, w) in enumerate(east_west(vals, lane32)):
                    k = g * GROUP + j
                    n = pltpu.roll(vals[j + 1], 1, 0)
                    s = pltpu.roll(vals[j + 1], 2 * ROWS - 1, 0)
                    pot[then, :, chunk(k)] = scaled[:, chunk(k)] + weight * ((e + w) + (n + s))
                return 0

            lax.fori_loop(0, n_chunks // GROUP, turn, 0)
            return 0

        lax.fori_loop(0, SWEEPS - 1, sweep, 0)

    solved = (SWEEPS - 1) % 2

    def update(k, e, w, column, to):
        n = pltpu.roll(column, 1, 0)[8:24]
        s = pltpu.roll(column, 2 * ROWS - 1, 0)[8:24]
        to(0, k, column[8:24].astype(BF16))
        to(1, k, (adv[1, :, chunk(k)].astype(F32) - 0.25 * (e - w)).astype(BF16))
        to(2, k, (adv[2, :, chunk(k)].astype(F32) - 0.25 * (s - n)).astype(BF16))

    def to_field(f, k, value):
        field[f, k] = value.astype(F32)

    def to_res(f, k, value):
        res[f, :, chunk(k)] = value

    def to_adv(f, k, value):
        adv[f, :, chunk(k)] = value

    def update_all():
        def turn(g, _):
            vals = around(g, lambda k: pot[solved, 8:24, chunk(k)])
            for j, (e, w) in enumerate(east_west(vals, lane)):
                k = g * GROUP + j
                update(k, e, w, pot[solved, :, chunk(k)], to_field)
            return 0

        lax.fori_loop(0, n_chunks // GROUP, turn, 0)

    def out_copy(part, peer):
        fs = slice(0, 3) if part == 0 else slice(3, 4)
        return pltpu.make_async_remote_copy(
            src_ref=res.at[fs, :, cols_of(peer)],
            dst_ref=out.at[fs, level, rows_of(block), :],
            send_sem=out_send.at[part],
            recv_sem=out_recv,
            device_id={"lon": peer, "lat": lat},
            device_id_type=MESH,
        )

    def out_keep(part):
        fs = slice(0, 3) if part == 0 else slice(3, 4)
        return pltpu.make_async_copy(
            res.at[fs, :, cols_of(lon)], out.at[fs, level, rows_of(block), :], out_recv
        )

    def update_and_send():
        per = tile // LANES

        def turn(j, _):
            peer = lax.rem(lon + j, n_lon)
            base = peer * per
            at = [lax.rem(base + i + n_chunks, n_chunks) for i in range(-1, per + 1)]
            vals = [pot[solved, 8:24, chunk(k)] for k in at]
            for i, (e, w) in enumerate(east_west(vals, lane)):
                k = base + i
                update(k, e, w, pot[solved, :, chunk(k)], to_res)

            @pl.when(j < n_lon)
            def _():
                out_copy(0, peer).start()

            return 0

        lax.fori_loop(1, n_lon + 1, turn, 0)
        out_keep(0).start()

    for step in range(STEPS):
        last = step == STEPS - 1
        if step == 0:
            wait_in(0)
            wait_in(1)
            unpack((0, 1, 2))
        else:
            wait_in(3)
        advect(step, range(3), [functools.partial(to_adv, f) for f in range(3)])
        sources(step)
        copies = halo_copies(step)
        for c in copies:
            c.start()
        if step == 0:
            wait_in(2)
            unpack((3,))
        advect(step, [3 + step], [functools.partial(to_res if last else to_field, 3 + (not last))])
        if last:

            def send_res3(j, _):
                out_copy(1, lax.rem(lon + j, n_lon)).start()
                return 0

            lax.fori_loop(1, n_lon, send_res3, 0)
            out_keep(1).start()
        for c in copies:
            c.wait_recv()
        complete(step)
        first_sweep()
        later_sweeps()
        if last:
            update_and_send()
        else:
            update_all()

    for part in range(4):
        wait_in_sent(part)
    for step in range(STEPS):
        for c in halo_copies(step):
            c.wait_send()
    sent = res.at[0:3, :, 0 : n_cols - tile]
    pltpu.make_async_copy(sent, sent, out_send.at[0]).wait()
    sent = res.at[3:4, :, 0 : n_cols - tile]
    pltpu.make_async_copy(sent, sent, out_send.at[1]).wait()
    pltpu.make_async_copy(out, out, out_recv).wait()


def local(n_lon, n_lat, fields, shifts, fractions, helm_coef):
    n_cols = n_lon * fields.shape[3]
    return pl.pallas_call(
        functools.partial(kernel, n_lon, n_lat),
        out_shape=jax.ShapeDtypeStruct(fields.shape, BF16),
        in_specs=[
            pl.BlockSpec(memory_space=pl.ANY),
            pl.BlockSpec(memory_space=pltpu.SMEM),
            pl.BlockSpec(memory_space=pl.ANY),
            pl.BlockSpec(memory_space=pltpu.SMEM),
        ],
        out_specs=pl.BlockSpec(memory_space=pl.ANY),
        scratch_shapes=[
            pltpu.VMEM((4, ROWS, n_cols), BF16),
            pltpu.VMEM((STEPS, ROWS, n_cols), F32),
            pltpu.VMEM((5, n_cols // LANES, ROWS, LANES), F32),
            pltpu.VMEM((3, ROWS, n_cols), BF16),
            pltpu.VMEM((4, ROWS, n_cols), BF16),
            pltpu.VMEM((3 * ROWS, n_cols), F32),
            pltpu.VMEM((2 * ROWS, n_cols), F32),
            pltpu.VMEM((2, 2 * ROWS, n_cols), F32),
            pltpu.VMEM((STEPS, ROWS, n_cols), BF16),
            pltpu.VMEM((STEPS, ROWS, n_cols), BF16),
            pltpu.VMEM((STEPS, ROWS, n_cols), BF16),
            pltpu.VMEM((STEPS, ROWS, n_cols), BF16),
            pltpu.SemaphoreType.DMA((4,)),
            pltpu.SemaphoreType.DMA((4,)),
            pltpu.SemaphoreType.DMA((STEPS, 2)),
            pltpu.SemaphoreType.DMA((STEPS, 2)),
            pltpu.SemaphoreType.DMA((2,)),
            pltpu.SemaphoreType.DMA,
        ],
        compiler_params=pltpu.CompilerParams(
            collective_id=0, has_side_effects=True, vmem_limit_bytes=32 * 2**20
        ),
        name="transport",
    )(fields, shifts, fractions, helm_coef)


def solution(mesh):
    return jax.shard_map(
        functools.partial(local, mesh.shape["lon"], mesh.shape["lat"]),
        mesh=mesh,
        in_specs=(P(None, None, "lat", "lon"), P(None, "lat"), P(None, "lat", "lon"), P()),
        out_specs=P(None, None, "lat", "lon"),
        check_vma=False,
    )
```

```python
import functools

import jax
import jax.numpy as jnp
from jax import lax
from jax.experimental import pallas as pl
from jax.experimental.pallas import tpu as pltpu
from jax.sharding import PartitionSpec as P

STEPS = 2
SWEEPS = 8
ROWS = 16
LANES = 128
GROUP = 16
F32 = jnp.float32
BF16 = jnp.bfloat16
MESH = pl.DeviceIdType.MESH


def place_of(lon):
    return 2 * (lon // 4) + lon % 2, (lon // 2) % 2


def lon_of(block, level):
    return 4 * (block // 2) + 2 * level + block % 2


def cubic_weights(a):
    am, ap, a2 = a - 1.0, a + 1.0, a - 2.0
    left, right = a * am, ap * a2
    return (
        left * a2 * (-1.0 / 6.0),
        right * am * 0.5,
        right * a * -0.5,
        ap * left * (1.0 / 6.0),
    )


def kernel(
    n_lon, n_lat, fields, shifts_hbm, fractions, helm_hbm, out,
    shifts, helm, x, frac, field, adv, north, res, src, scaled, pot, down, up, above, below,
    small, in_send, in_recv, halo_send, halo_recv, out_send, out_recv,
):
    n_cols = n_lon * fields.shape[3]
    tile = fields.shape[3]
    n_chunks = n_cols // LANES
    n_blocks = fields.shape[2] // ROWS
    lon, lat = lax.axis_index("lon"), lax.axis_index("lat")
    block, level = place_of(lon)

    prev_block = lax.rem(block + n_blocks - 1, n_blocks)
    next_block = lax.rem(block + 1, n_blocks)
    lat_up = lax.rem(lat + n_lat - (block == 0).astype(jnp.int32), n_lat)
    lat_down = lax.rem(lat + (block == n_blocks - 1).astype(jnp.int32), n_lat)
    dev_up = {"lon": lon_of(prev_block, level), "lat": lat_up}
    dev_down = {"lon": lon_of(next_block, level), "lat": lat_down}
    row_block = lat * n_blocks + block
    has_above = row_block > 0
    has_below = row_block < n_lat * n_blocks - 1

    def rows_of(b):
        return pl.ds(pl.multiple_of(b * ROWS, ROWS), ROWS)

    def cols_of(p):
        return pl.ds(pl.multiple_of(p * tile, tile), tile)

    def chunk(k):
        return pl.ds(pl.multiple_of(k * LANES, LANES), LANES)

    def wrap(k):
        return k & (n_chunks - 1)

    def each_group(turn):
        def body(g, _):
            turn(g * GROUP)
            return 0

        lax.fori_loop(0, n_chunks // GROUP, body, 0)

    barrier = pltpu.get_barrier_semaphore()

    def greet(j, _):
        peer = lax.rem(lon + j, n_lon)
        pl.semaphore_signal(barrier, inc=1, device_id={"lon": peer, "lat": lat}, device_id_type=MESH)
        return 0

    lax.fori_loop(1, n_lon, greet, 0)
    pl.semaphore_signal(barrier, inc=1, device_id=dev_up, device_id_type=MESH)
    pl.semaphore_signal(barrier, inc=1, device_id=dev_down, device_id_type=MESH)

    get_shifts = pltpu.make_async_copy(shifts_hbm, shifts, small.at[0])
    get_helm = pltpu.make_async_copy(helm_hbm, helm, small.at[1])
    get_shifts.start()
    get_helm.start()

    zero = jnp.zeros((8, LANES), F32)

    def clear(base):
        for j in range(GROUP):
            k = base + j
            north[k, 0:8] = zero
            north[k, 24:32] = zero
            for i in range(2):
                pot[i, k, 0:8] = zero
                pot[i, k, 40:48] = zero

    each_group(clear)
    pl.semaphore_wait(barrier, n_lon + 1)

    def in_refs(part, to_block, to_level, from_lon):
        if part == 0:
            return (fields.at[0:3, to_level, rows_of(to_block), :], x.at[0:3, :, cols_of(from_lon)])
        if part == 2:
            return (fields.at[3, to_level, rows_of(to_block), :], x.at[3, :, cols_of(from_lon)])
        step = part // 2
        return (fractions.at[step, rows_of(to_block), :], frac.at[step, :, cols_of(from_lon)])

    def send_parts(parts):
        def turn(j, _):
            peer = lax.rem(lon + j, n_lon)
            to_block, to_level = place_of(peer)
            for part in parts:
                from_ref, to_ref = in_refs(part, to_block, to_level, lon)
                pltpu.make_async_remote_copy(
                    src_ref=from_ref,
                    dst_ref=to_ref,
                    send_sem=in_send.at[part],
                    recv_sem=in_recv.at[part],
                    device_id={"lon": peer, "lat": lat},
                    device_id_type=MESH,
                ).start()
            return 0

        lax.fori_loop(1, n_lon, turn, 0)
        for part in parts:
            from_ref, to_ref = in_refs(part, block, level, lon)
            pltpu.make_async_copy(from_ref, to_ref, in_recv.at[part]).start()

    def in_whole(part):
        return (x.at[0:3], frac.at[0], x.at[3], frac.at[1])[part]

    def wait_in(part):
        whole = in_whole(part)
        pltpu.make_async_copy(whole, whole, in_recv.at[part]).wait()

    def wait_in_sent(part):
        whole = in_whole(part)
        sent = whole.at[:, :, 0 : n_cols - tile] if part == 0 else whole.at[:, 0 : n_cols - tile]
        pltpu.make_async_copy(sent, sent, in_send.at[part]).wait()

    send_parts((0, 1))
    send_parts((2, 3))
    get_shifts.wait()
    get_helm.wait()

    lane16 = lax.broadcasted_iota(jnp.int32, (ROWS, LANES), 1)
    row8 = lax.broadcasted_iota(jnp.int32, (8, LANES), 0)

    def weight_of(start, rows):
        row = start + lax.broadcasted_iota(jnp.int32, (rows, LANES), 0)
        coef = jnp.full((rows, LANES), helm[level], F32)
        inverse = 1.0 / (1.0 + 4.0 * coef)
        inside = ((row >= ROWS) | has_above) & ((row < 2 * ROWS) | has_below)
        return jnp.where(inside, coef * inverse, 0.0), inverse

    def unpack(parts):
        def turn(base):
            for j in range(GROUP):
                for f in parts:
                    field[f, base + j] = x[f, :, chunk(base + j)].astype(F32)

        each_group(turn)

    def advect(step, sources, targets):
        shift = shifts[step, block]
        taps = []
        for d in (1, 0, -1, -2):
            total = (shift + (n_cols - d)) & (n_cols - 1)
            taps.append((total // LANES, total & (LANES - 1)))
        from_here = [lane16 >= part for _, part in taps]

        def turn(base):
            weights = [cubic_weights(frac[step, :, chunk(base + j)]) for j in range(GROUP)]
            for f, to in zip(sources, targets):
                total = [None] * GROUP
                for tap, (whole, part) in enumerate(taps):
                    before = None
                    for j in range(-1, GROUP):
                        here = pltpu.roll(field[f, wrap(base + j - whole + n_chunks)], part, 1)
                        if j >= 0:
                            term = weights[j][tap] * jnp.where(from_here[tap], here, before)
                            total[j] = term if tap == 0 else total[j] + term
                        before = here
                for j in range(GROUP):
                    to(base + j, total[j].astype(BF16))

        each_group(turn)

    def east_west(base, count, load):
        vals = [load(wrap(base - 1 + n_chunks))] + [load(base + j) for j in range(count)]
        vals.append(load(wrap(base + count)))
        ln = lax.broadcasted_iota(jnp.int32, vals[0].shape, 1)
        last, first = ln == LANES - 1, ln == 0
        east = [None] + [pltpu.roll(v, LANES - 1, 1) for v in vals[1:]]
        west = [pltpu.roll(v, 1, 1) for v in vals[:-1]]
        return [
            (vals[j], jnp.where(last, east[j + 1], east[j]), jnp.where(first, west[j - 1], west[j]))
            for j in range(1, count + 1)
        ]

    def sources(step):
        def turn(base):
            for j, (_, e, w) in enumerate(east_west(base, GROUP, lambda k: adv[1, k])):
                k = base + j
                own = adv[0, k] - 0.25 * ((e - w) + (north[k, 9:25] - north[k, 7:23]))
                src[k, ROWS : 2 * ROWS] = own
                top, bottom = own[0:8], own[8:16]
                with_last = jnp.where(row8 == 0, north[k, 23:31], top)
                with_first = jnp.where(row8 == 7, north[k, 1:9], bottom)
                down[step, k] = jnp.concatenate([with_last, bottom], axis=0).astype(BF16)
                up[step, k] = jnp.concatenate([top, with_first], axis=0).astype(BF16)

        each_group(turn)

    def halo_copies(step):
        return (
            pltpu.make_async_remote_copy(
                src_ref=down.at[step],
                dst_ref=above.at[step],
                send_sem=halo_send.at[step, 0],
                recv_sem=halo_recv.at[step, 0],
                device_id=dev_down,
                device_id_type=MESH,
            ),
            pltpu.make_async_remote_copy(
                src_ref=up.at[step],
                dst_ref=below.at[step],
                send_sem=halo_send.at[step, 1],
                recv_sem=halo_recv.at[step, 1],
                device_id=dev_up,
                device_id_type=MESH,
            ),
        )

    def complete(step):
        first_has, last_has = (row8 == 0) & has_below, (row8 == 7) & has_above

        def turn(base):
            for j in range(GROUP):
                k = base + j
                a = jnp.where(has_above, above[step, k].astype(F32), 0.0)
                b = jnp.where(has_below, below[step, k].astype(F32), 0.0)
                src[k, 0:8] = a[0:8]
                src[k, 8:16] = a[8:16] - jnp.where(last_has, 0.25 * north[k, 1:9], 0.0)
                src[k, 16:24] = src[k, 16:24] + jnp.where(row8 == 0, 0.25 * a[0:8], 0.0)
                src[k, 24:32] = src[k, 24:32] - jnp.where(row8 == 7, 0.25 * b[8:16], 0.0)
                src[k, 32:40] = b[0:8] + jnp.where(first_has, 0.25 * north[k, 23:31], 0.0)
                src[k, 40:48] = b[8:16]

        each_group(turn)

    def first_sweep():
        weight, inverse = weight_of(8, 2 * ROWS)

        def turn(base):
            for j, (mid, e, w) in enumerate(east_west(base, GROUP, lambda k: src[k, 8:40])):
                k = base + j
                fixed = mid * inverse
                scaled[k] = fixed
                pot[0, k, 8:40] = fixed + weight * ((e + w) + (src[k, 7:39] + src[k, 9:41]))

        each_group(turn)

    def later_sweeps(begin, end, start, rows):
        weight, _ = weight_of(start, rows)

        def sweep(i, _):
            now, then = i & 1, (i + 1) & 1

            def turn(base):
                for j, (_, e, w) in enumerate(
                    east_west(base, GROUP, lambda k: pot[now, k, start : start + rows])
                ):
                    k = base + j
                    n = pot[now, k, start - 1 : start - 1 + rows]
                    s = pot[now, k, start + 1 : start + 1 + rows]
                    fixed = scaled[k, start - 8 : start - 8 + rows]
                    pot[then, k, start : start + rows] = fixed + weight * ((e + w) + (n + s))

            each_group(turn)
            return 0

        lax.fori_loop(begin, end, sweep, 0)

    solved = (SWEEPS - 1) % 2

    def update(base, count, to):
        own = east_west(base, count, lambda k: pot[solved, k, ROWS : 2 * ROWS])
        for j, (mid, e, w) in enumerate(own):
            k = base + j
            n, s = pot[solved, k, ROWS - 1 : 2 * ROWS - 1], pot[solved, k, ROWS + 1 : 2 * ROWS + 1]
            to(0, k, mid.astype(BF16))
            to(1, k, (adv[1, k] - 0.25 * (e - w)).astype(BF16))
            to(2, k, (north[k, 8:24] - 0.25 * (s - n)).astype(BF16))

    def to_field(f, k, value):
        field[f, k] = value.astype(F32)

    def to_res(f, k, value):
        res[f, :, chunk(k)] = value

    def to_adv(f, k, value):
        if f == 2:
            north[k, 8:24] = value.astype(F32)
        else:
            adv[f, k] = value.astype(F32)

    def out_copy(part, peer):
        fs = slice(0, 3) if part == 0 else slice(3, 4)
        return pltpu.make_async_remote_copy(
            src_ref=res.at[fs, :, cols_of(peer)],
            dst_ref=out.at[fs, level, rows_of(block), :],
            send_sem=out_send.at[part],
            recv_sem=out_recv,
            device_id={"lon": peer, "lat": lat},
            device_id_type=MESH,
        )

    def out_keep(part):
        fs = slice(0, 3) if part == 0 else slice(3, 4)
        return pltpu.make_async_copy(
            res.at[fs, :, cols_of(lon)], out.at[fs, level, rows_of(block), :], out_recv
        )

    def update_and_send():
        per = tile // LANES

        def turn(j, _):
            peer = lax.rem(lon + j, n_lon)
            update(peer * per, per, to_res)

            @pl.when(j < n_lon)
            def _():
                out_copy(0, peer).start()

            return 0

        lax.fori_loop(1, n_lon + 1, turn, 0)
        out_keep(0).start()

    for step in range(STEPS):
        last = step == STEPS - 1
        if step == 0:
            wait_in(0)
            wait_in(1)
            unpack((0, 1, 2))
        else:
            wait_in(3)
        advect(step, range(3), [functools.partial(to_adv, f) for f in range(3)])
        sources(step)
        copies = halo_copies(step)
        for c in copies:
            c.start()
        if step == 0:
            wait_in(2)
            unpack((3,))
        advect(step, [3 + step], [functools.partial(to_res if last else to_field, 3 + (not last))])
        if last:

            def send_res3(j, _):
                out_copy(1, lax.rem(lon + j, n_lon)).start()
                return 0

            lax.fori_loop(1, n_lon, send_res3, 0)
            out_keep(1).start()
        for c in copies:
            c.wait_recv()
        complete(step)
        first_sweep()
        later_sweeps(0, 3, 8, 32)
        later_sweeps(3, SWEEPS - 1, 12, 24)
        if last:
            update_and_send()
        else:
            each_group(lambda base: update(base, GROUP, to_field))

    for part in range(4):
        wait_in_sent(part)
    for step in range(STEPS):
        for c in halo_copies(step):
            c.wait_send()
    sent = res.at[0:3, :, 0 : n_cols - tile]
    pltpu.make_async_copy(sent, sent, out_send.at[0]).wait()
    sent = res.at[3:4, :, 0 : n_cols - tile]
    pltpu.make_async_copy(sent, sent, out_send.at[1]).wait()
    pltpu.make_async_copy(out, out, out_recv).wait()


def local(n_lon, n_lat, fields, shifts, fractions, helm_coef):
    n_cols = n_lon * fields.shape[3]
    n_chunks = n_cols // LANES
    return pl.pallas_call(
        functools.partial(kernel, n_lon, n_lat),
        out_shape=jax.ShapeDtypeStruct(fields.shape, BF16),
        in_specs=[pl.BlockSpec(memory_space=pltpu.HBM)] * 4,
        out_specs=pl.BlockSpec(memory_space=pl.ANY),
        scratch_shapes=[
            pltpu.SMEM(shifts.shape, jnp.int32),
            pltpu.SMEM(helm_coef.shape, F32),
            pltpu.VMEM((4, ROWS, n_cols), BF16),
            pltpu.VMEM((STEPS, ROWS, n_cols), F32),
            pltpu.VMEM((5, n_chunks, ROWS, LANES), F32),
            pltpu.VMEM((2, n_chunks, ROWS, LANES), F32),
            pltpu.VMEM((n_chunks, 2 * ROWS, LANES), F32),
            pltpu.VMEM((4, ROWS, n_cols), BF16),
            pltpu.VMEM((n_chunks, 3 * ROWS, LANES), F32),
            pltpu.VMEM((n_chunks, 2 * ROWS, LANES), F32),
            pltpu.VMEM((2, n_chunks, 3 * ROWS, LANES), F32),
            pltpu.VMEM((STEPS, n_chunks, ROWS, LANES), BF16),
            pltpu.VMEM((STEPS, n_chunks, ROWS, LANES), BF16),
            pltpu.VMEM((STEPS, n_chunks, ROWS, LANES), BF16),
            pltpu.VMEM((STEPS, n_chunks, ROWS, LANES), BF16),
            pltpu.SemaphoreType.DMA((2,)),
            pltpu.SemaphoreType.DMA((4,)),
            pltpu.SemaphoreType.DMA((4,)),
            pltpu.SemaphoreType.DMA((STEPS, 2)),
            pltpu.SemaphoreType.DMA((STEPS, 2)),
            pltpu.SemaphoreType.DMA((2,)),
            pltpu.SemaphoreType.DMA,
        ],
        compiler_params=pltpu.CompilerParams(
            collective_id=0, has_side_effects=True, vmem_limit_bytes=32 * 2**20
        ),
        name="transport",
    )(*[pltpu.with_memory_space_constraint(a, pltpu.HBM) for a in (fields, shifts, fractions, helm_coef)])


def solution(mesh):
    return jax.shard_map(
        functools.partial(local, mesh.shape["lon"], mesh.shape["lat"]),
        mesh=mesh,
        in_specs=(P(None, None, "lat", "lon"), P(None, "lat"), P(None, "lat", "lon"), P()),
        out_specs=P(None, None, "lat", "lon"),
        check_vma=False,
    )
```

```python
import functools

import jax
import jax.numpy as jnp
from jax import lax
from jax.experimental import pallas as pl
from jax.experimental.pallas import tpu as pltpu
from jax.sharding import PartitionSpec as P

STEPS = 2
SWEEPS = 8
ROWS = 16
LANES = 128
F32 = jnp.float32
BF16 = jnp.bfloat16
UNITS, HALF = 65535.0, 32768
MESH = pl.DeviceIdType.MESH


def place_of(lon):
    return 2 * (lon // 4) + lon % 2, (lon // 2) % 2


def lon_of(block, level):
    return 4 * (block // 2) + 2 * level + block % 2


def cubic_weights(a):
    am, ap, a2 = a - 1.0, a + 1.0, a - 2.0
    left, right = a * am, ap * a2
    return (
        left * a2 * (-1.0 / 6.0),
        right * am * 0.5,
        right * a * -0.5,
        ap * left * (1.0 / 6.0),
    )


def kernel(
    n_lon, n_lat, fields, shifts_hbm, fractions, helm_hbm, out,
    shifts, helm, raw, coded, x, frac, field, adv, north, res, src, scaled, pot, down, up, above, below,
    small, in_send, in_recv, halo_send, halo_recv, out_send, out_recv,
):
    n_cols = n_lon * fields.shape[3]
    tile = fields.shape[3]
    n_chunks = n_cols // LANES
    n_blocks = fields.shape[2] // ROWS
    lon, lat = lax.axis_index("lon"), lax.axis_index("lat")
    block, level = place_of(lon)

    prev_block = lax.rem(block + n_blocks - 1, n_blocks)
    next_block = lax.rem(block + 1, n_blocks)
    lat_up = lax.rem(lat + n_lat - (block == 0).astype(jnp.int32), n_lat)
    lat_down = lax.rem(lat + (block == n_blocks - 1).astype(jnp.int32), n_lat)
    dev_up = {"lon": lon_of(prev_block, level), "lat": lat_up}
    dev_down = {"lon": lon_of(next_block, level), "lat": lat_down}
    row_block = lat * n_blocks + block
    has_above = row_block > 0
    has_below = row_block < n_lat * n_blocks - 1

    def rows_of(b):
        return pl.ds(pl.multiple_of(b * ROWS, ROWS), ROWS)

    def cols_of(p):
        return pl.ds(pl.multiple_of(p * tile, tile), tile)

    def chunk(k):
        return pl.ds(pl.multiple_of(k * LANES, LANES), LANES)

    def wrap(k):
        return k & (n_chunks - 1)

    barrier = pltpu.get_barrier_semaphore()

    def greet(j, _):
        peer = lax.rem(lon + j, n_lon)
        pl.semaphore_signal(barrier, inc=1, device_id={"lon": peer, "lat": lat}, device_id_type=MESH)
        return 0

    lax.fori_loop(1, n_lon, greet, 0)
    pl.semaphore_signal(barrier, inc=1, device_id=dev_up, device_id_type=MESH)
    pl.semaphore_signal(barrier, inc=1, device_id=dev_down, device_id_type=MESH)

    get_shifts = pltpu.make_async_copy(shifts_hbm, shifts, small.at[0])
    get_helm = pltpu.make_async_copy(helm_hbm, helm, small.at[1])
    get_fractions = [
        pltpu.make_async_copy(fractions.at[step], raw.at[step], small.at[2 + step]) for step in range(STEPS)
    ]
    for c in get_fractions:
        c.start()
    get_shifts.start()
    get_helm.start()

    zero = jnp.zeros((8, LANES), F32)

    def clear(base):
        for j in range(n_chunks):
            k = base + j
            north[k, 0:8] = zero
            north[k, 24:32] = zero
            for i in range(2):
                pot[i, k, 0:8] = zero
                pot[i, k, 40:48] = zero

    clear(0)
    pl.semaphore_wait(barrier, n_lon + 1)

    def in_refs(part, to_block, to_level, from_lon):
        if part < 4:
            return (fields.at[part, to_level, rows_of(to_block), :], x.at[part, :, cols_of(from_lon)])
        return (coded.at[part - 4, rows_of(to_block), :], frac.at[part - 4, :, cols_of(from_lon)])

    def send_part(part):
        def turn(j, _):
            peer = lax.rem(lon + j, n_lon)
            to_block, to_level = place_of(peer)
            from_ref, to_ref = in_refs(part, to_block, to_level, lon)
            pltpu.make_async_remote_copy(
                src_ref=from_ref,
                dst_ref=to_ref,
                send_sem=in_send.at[part],
                recv_sem=in_recv.at[part],
                device_id={"lon": peer, "lat": lat},
                device_id_type=MESH,
            ).start()
            return 0

        lax.fori_loop(1, n_lon, turn, 0)
        from_ref, to_ref = in_refs(part, block, level, lon)
        pltpu.make_async_copy(from_ref, to_ref, in_recv.at[part]).start()

    def in_whole(part):
        return x.at[part] if part < 4 else frac.at[part - 4]

    def wait_in(part):
        whole = in_whole(part)
        pltpu.make_async_copy(whole, whole, in_recv.at[part]).wait()

    def wait_in_sent(part):
        sent = in_whole(part).at[:, 0 : n_cols - tile]
        pltpu.make_async_copy(sent, sent, in_send.at[part]).wait()

    def code(step):
        get_fractions[step].wait()
        coded[step] = ((raw[step] * UNITS + 0.5).astype(jnp.int32) - HALF).astype(jnp.int16)

    def decode(value):
        return value.astype(jnp.int32).astype(F32) * (1.0 / UNITS) + HALF / UNITS

    send_part(0)
    code(0)
    send_part(4)
    send_part(1)
    send_part(2)
    code(1)
    send_part(3)
    send_part(5)
    get_shifts.wait()
    get_helm.wait()

    lane16 = lax.broadcasted_iota(jnp.int32, (ROWS, LANES), 1)
    row8 = lax.broadcasted_iota(jnp.int32, (8, LANES), 0)

    def weight_of(start, rows):
        row = start + lax.broadcasted_iota(jnp.int32, (rows, LANES), 0)
        coef = jnp.full((rows, LANES), helm[level], F32)
        inverse = 1.0 / (1.0 + 4.0 * coef)
        inside = ((row >= ROWS) | has_above) & ((row < 2 * ROWS) | has_below)
        return jnp.where(inside, coef * inverse, 0.0), inverse

    def unpack(parts):
        def turn(base):
            for j in range(n_chunks):
                for f in parts:
                    field[f, base + j] = x[f, :, chunk(base + j)].astype(F32)

        turn(0)

    def advect(step, sources, targets):
        shift = shifts[step, block]
        taps = []
        for d in (1, 0, -1, -2):
            total = (shift + (n_cols - d)) & (n_cols - 1)
            taps.append((total // LANES, total & (LANES - 1)))
        from_here = [lane16 >= part for _, part in taps]

        def turn(base):
            weights = [cubic_weights(decode(frac[step, :, chunk(base + j)])) for j in range(n_chunks)]
            for f, to in zip(sources, targets):
                total = [None] * n_chunks
                for tap, (whole, part) in enumerate(taps):
                    before = None
                    for j in range(-1, n_chunks):
                        here = pltpu.roll(field[f, wrap(base + j - whole + n_chunks)], part, 1)
                        if j >= 0:
                            term = weights[j][tap] * jnp.where(from_here[tap], here, before)
                            total[j] = term if tap == 0 else total[j] + term
                        before = here
                for j in range(n_chunks):
                    to(base + j, total[j].astype(BF16))

        turn(0)

    def east_west(base, count, load):
        mid = load(base)
        ln = lax.broadcasted_iota(jnp.int32, mid.shape, 1)
        last, first = ln == LANES - 1, ln == 0
        before = pltpu.roll(load(wrap(base - 1 + n_chunks)), 1, 1)
        mid_east = pltpu.roll(mid, LANES - 1, 1)
        for j in range(count):
            after = load(wrap(base + j + 1))
            after_east = pltpu.roll(after, LANES - 1, 1)
            mid_west = pltpu.roll(mid, 1, 1)
            yield (
                base + j,
                mid,
                jnp.where(last, after_east, mid_east),
                jnp.where(first, before, mid_west),
            )
            mid, mid_east, before = after, after_east, mid_west

    def sources(step):
        def turn(base):
            for k, _, e, w in east_west(base, n_chunks, lambda k: adv[1, k]):
                own = adv[0, k] - 0.25 * ((e - w) + (north[k, 9:25] - north[k, 7:23]))
                src[k, ROWS : 2 * ROWS] = own
                top, bottom = own[0:8], own[8:16]
                with_last = jnp.where(row8 == 0, north[k, 23:31], top)
                with_first = jnp.where(row8 == 7, north[k, 1:9], bottom)
                down[step, k] = jnp.concatenate([with_last, bottom], axis=0).astype(BF16)
                up[step, k] = jnp.concatenate([top, with_first], axis=0).astype(BF16)

        turn(0)

    def halo_copies(step):
        return (
            pltpu.make_async_remote_copy(
                src_ref=down.at[step],
                dst_ref=above.at[step],
                send_sem=halo_send.at[step, 0],
                recv_sem=halo_recv.at[step, 0],
                device_id=dev_down,
                device_id_type=MESH,
            ),
            pltpu.make_async_remote_copy(
                src_ref=up.at[step],
                dst_ref=below.at[step],
                send_sem=halo_send.at[step, 1],
                recv_sem=halo_recv.at[step, 1],
                device_id=dev_up,
                device_id_type=MESH,
            ),
        )

    def complete(step):
        first_has, last_has = (row8 == 0) & has_below, (row8 == 7) & has_above

        def turn(base):
            for j in range(n_chunks):
                k = base + j
                a = jnp.where(has_above, above[step, k].astype(F32), 0.0)
                b = jnp.where(has_below, below[step, k].astype(F32), 0.0)
                src[k, 0:8] = a[0:8]
                src[k, 8:16] = a[8:16] - jnp.where(last_has, 0.25 * north[k, 1:9], 0.0)
                src[k, 16:24] = src[k, 16:24] + jnp.where(row8 == 0, 0.25 * a[0:8], 0.0)
                src[k, 24:32] = src[k, 24:32] - jnp.where(row8 == 7, 0.25 * b[8:16], 0.0)
                src[k, 32:40] = b[0:8] + jnp.where(first_has, 0.25 * north[k, 23:31], 0.0)
                src[k, 40:48] = b[8:16]

        turn(0)

    def first_sweep():
        weight, inverse = weight_of(8, 2 * ROWS)

        def turn(base):
            for k, mid, e, w in east_west(base, n_chunks, lambda k: src[k, 8:40]):
                fixed = mid * inverse
                scaled[k] = fixed
                pot[0, k, 8:40] = fixed + weight * ((e + w) + (src[k, 7:39] + src[k, 9:41]))

        turn(0)

    def later_sweeps():
        def sweep(now, start, weight):
            rows = weight.shape[0]
            for k, _, e, w in east_west(0, n_chunks, lambda k: pot[now, k, start : start + rows]):
                n = pot[now, k, start - 1 : start - 1 + rows]
                s = pot[now, k, start + 1 : start + 1 + rows]
                fixed = scaled[k, start - 8 : start - 8 + rows]
                pot[1 - now, k, start : start + rows] = fixed + weight * ((e + w) + (n + s))

        wide, _ = weight_of(8, 32)
        narrow, _ = weight_of(12, 24)

        def pair(i, _):
            sweep(0, 8, wide)
            sweep(1, 8, wide)
            return 0

        lax.fori_loop(0, 2, pair, 0)
        for i in range(4, SWEEPS - 1):
            sweep(i % 2, 12, narrow)

    solved = (SWEEPS - 1) % 2

    def update(base, count, to):
        for k, mid, e, w in east_west(base, count, lambda k: pot[solved, k, ROWS : 2 * ROWS]):
            n, s = pot[solved, k, ROWS - 1 : 2 * ROWS - 1], pot[solved, k, ROWS + 1 : 2 * ROWS + 1]
            to(0, k, mid.astype(BF16))
            to(1, k, (adv[1, k] - 0.25 * (e - w)).astype(BF16))
            to(2, k, (north[k, 8:24] - 0.25 * (s - n)).astype(BF16))

    def to_field(f, k, value):
        field[f, k] = value.astype(F32)

    def to_res(f, k, value):
        res[f, :, chunk(k)] = value

    def to_adv(f, k, value):
        if f == 2:
            north[k, 8:24] = value.astype(F32)
        else:
            adv[f, k] = value.astype(F32)

    def out_copy(part, peer):
        fs = slice(0, 3) if part == 0 else slice(3, 4)
        return pltpu.make_async_remote_copy(
            src_ref=res.at[fs, :, cols_of(peer)],
            dst_ref=out.at[fs, level, rows_of(block), :],
            send_sem=out_send.at[part],
            recv_sem=out_recv,
            device_id={"lon": peer, "lat": lat},
            device_id_type=MESH,
        )

    def out_keep(part):
        fs = slice(0, 3) if part == 0 else slice(3, 4)
        return pltpu.make_async_copy(
            res.at[fs, :, cols_of(lon)], out.at[fs, level, rows_of(block), :], out_recv
        )

    def update_and_send():
        per = tile // LANES

        def turn(j, _):
            peer = lax.rem(lon + j, n_lon)
            update(peer * per, per, to_res)

            @pl.when(j < n_lon)
            def _():
                out_copy(0, peer).start()

            return 0

        lax.fori_loop(1, n_lon + 1, turn, 0)
        out_keep(0).start()

    for step in range(STEPS):
        last = step == STEPS - 1
        if step == 0:
            wait_in(4)
            for f in range(3):
                wait_in(f)
                unpack((f,))
                advect(step, [f], [functools.partial(to_adv, f)])
        else:
            wait_in(5)
            advect(step, range(3), [functools.partial(to_adv, f) for f in range(3)])
        sources(step)
        copies = halo_copies(step)
        for c in copies:
            c.start()
        if step == 0:
            wait_in(3)
            unpack((3,))
        advect(step, [3 + step], [functools.partial(to_res if last else to_field, 3 + (not last))])
        if last:

            def send_res3(j, _):
                out_copy(1, lax.rem(lon + j, n_lon)).start()
                return 0

            lax.fori_loop(1, n_lon, send_res3, 0)
            out_keep(1).start()
        for c in copies:
            c.wait_recv()
        complete(step)
        first_sweep()
        later_sweeps()
        if last:
            update_and_send()
        else:
            update(0, n_chunks, to_field)

    for part in range(6):
        wait_in_sent(part)
    for step in range(STEPS):
        for c in halo_copies(step):
            c.wait_send()
    sent = res.at[0:3, :, 0 : n_cols - tile]
    pltpu.make_async_copy(sent, sent, out_send.at[0]).wait()
    sent = res.at[3:4, :, 0 : n_cols - tile]
    pltpu.make_async_copy(sent, sent, out_send.at[1]).wait()
    pltpu.make_async_copy(out, out, out_recv).wait()


def local(n_lon, n_lat, fields, shifts, fractions, helm_coef):
    n_cols = n_lon * fields.shape[3]
    n_chunks = n_cols // LANES
    return pl.pallas_call(
        functools.partial(kernel, n_lon, n_lat),
        out_shape=jax.ShapeDtypeStruct(fields.shape, BF16),
        in_specs=[pl.BlockSpec(memory_space=pltpu.HBM)] * 4,
        out_specs=pl.BlockSpec(memory_space=pl.ANY),
        scratch_shapes=[
            pltpu.SMEM(shifts.shape, jnp.int32),
            pltpu.SMEM(helm_coef.shape, F32),
            pltpu.VMEM(fractions.shape, F32),
            pltpu.VMEM(fractions.shape, jnp.int16),
            pltpu.VMEM((4, ROWS, n_cols), BF16),
            pltpu.VMEM((STEPS, ROWS, n_cols), jnp.int16),
            pltpu.VMEM((5, n_chunks, ROWS, LANES), F32),
            pltpu.VMEM((2, n_chunks, ROWS, LANES), F32),
            pltpu.VMEM((n_chunks, 2 * ROWS, LANES), F32),
            pltpu.VMEM((4, ROWS, n_cols), BF16),
            pltpu.VMEM((n_chunks, 3 * ROWS, LANES), F32),
            pltpu.VMEM((n_chunks, 2 * ROWS, LANES), F32),
            pltpu.VMEM((2, n_chunks, 3 * ROWS, LANES), F32),
            pltpu.VMEM((STEPS, n_chunks, ROWS, LANES), BF16),
            pltpu.VMEM((STEPS, n_chunks, ROWS, LANES), BF16),
            pltpu.VMEM((STEPS, n_chunks, ROWS, LANES), BF16),
            pltpu.VMEM((STEPS, n_chunks, ROWS, LANES), BF16),
            pltpu.SemaphoreType.DMA((2 + STEPS,)),
            pltpu.SemaphoreType.DMA((4 + STEPS,)),
            pltpu.SemaphoreType.DMA((4 + STEPS,)),
            pltpu.SemaphoreType.DMA((STEPS, 2)),
            pltpu.SemaphoreType.DMA((STEPS, 2)),
            pltpu.SemaphoreType.DMA((2,)),
            pltpu.SemaphoreType.DMA,
        ],
        compiler_params=pltpu.CompilerParams(
            collective_id=0, has_side_effects=True, vmem_limit_bytes=32 * 2**20
        ),
        name="transport",
    )(*[pltpu.with_memory_space_constraint(a, pltpu.HBM) for a in (fields, shifts, fractions, helm_coef)])


def solution(mesh):
    return jax.shard_map(
        functools.partial(local, mesh.shape["lon"], mesh.shape["lat"]),
        mesh=mesh,
        in_specs=(P(None, None, "lat", "lon"), P(None, "lat"), P(None, "lat", "lon"), P()),
        out_specs=P(None, None, "lat", "lon"),
        check_vma=False,
    )
```

```python
import functools

import jax
import jax.numpy as jnp
from jax import lax
from jax.experimental import pallas as pl
from jax.experimental.pallas import tpu as pltpu
from jax.sharding import PartitionSpec as P

STEPS = 2
SWEEPS = 8
ROWS = 16
LANES = 128
F32 = jnp.float32
BF16 = jnp.bfloat16
UNITS, HALF = 65535.0, 32768
MESH = pl.DeviceIdType.MESH


def place_of(lon, lat, n_blocks):
    along = 2 * lax.div(lon, 4) + lax.rem(lon, 2)
    odd = lax.rem(lat, 2)
    return along + odd * (n_blocks - 1 - 2 * along), lax.rem(lax.div(lon, 2), 2)


def lon_of(block, level, lat, n_blocks):
    odd = lax.rem(lat, 2)
    along = block + odd * (n_blocks - 1 - 2 * block)
    return 4 * lax.div(along, 2) + 2 * level + lax.rem(along, 2)


def cubic_weights(a):
    am, ap, a2 = a - 1.0, a + 1.0, a - 2.0
    left, right = a * am, ap * a2
    return (
        left * a2 * (-1.0 / 6.0),
        right * am * 0.5,
        right * a * -0.5,
        ap * left * (1.0 / 6.0),
    )


def kernel(
    n_lon, n_lat, fields, shifts_hbm, fractions, helm_hbm, out,
    shifts, helm, raw, coded, x, frac, field, adv, north, res, src, scaled, pot, down, up, above, below,
    small, in_send, in_recv, halo_send, halo_recv, out_send, out_recv,
):
    n_cols = n_lon * fields.shape[3]
    tile = fields.shape[3]
    n_chunks = n_cols // LANES
    n_blocks = fields.shape[2] // ROWS
    lon, lat = lax.axis_index("lon"), lax.axis_index("lat")
    block, level = place_of(lon, lat, n_blocks)

    prev_block = lax.rem(block + n_blocks - 1, n_blocks)
    next_block = lax.rem(block + 1, n_blocks)
    lat_up = lax.rem(lat + n_lat - (block == 0).astype(jnp.int32), n_lat)
    lat_down = lax.rem(lat + (block == n_blocks - 1).astype(jnp.int32), n_lat)
    dev_up = {"lon": lon_of(prev_block, level, lat_up, n_blocks), "lat": lat_up}
    dev_down = {"lon": lon_of(next_block, level, lat_down, n_blocks), "lat": lat_down}
    row_block = lat * n_blocks + block
    has_above = row_block > 0
    has_below = row_block < n_lat * n_blocks - 1

    def rows_of(b):
        return pl.ds(pl.multiple_of(b * ROWS, ROWS), ROWS)

    def cols_of(p):
        return pl.ds(pl.multiple_of(p * tile, tile), tile)

    def chunk(k):
        return pl.ds(pl.multiple_of(k * LANES, LANES), LANES)

    def wrap(k):
        return k & (n_chunks - 1)

    barrier = pltpu.get_barrier_semaphore()

    def greet(j, _):
        peer = lax.rem(lon + j, n_lon)
        pl.semaphore_signal(barrier, inc=1, device_id={"lon": peer, "lat": lat}, device_id_type=MESH)
        return 0

    lax.fori_loop(1, n_lon, greet, 0)
    pl.semaphore_signal(barrier, inc=1, device_id=dev_up, device_id_type=MESH)
    pl.semaphore_signal(barrier, inc=1, device_id=dev_down, device_id_type=MESH)

    get_shifts = pltpu.make_async_copy(shifts_hbm, shifts, small.at[0])
    get_helm = pltpu.make_async_copy(helm_hbm, helm, small.at[1])
    get_fractions = [
        pltpu.make_async_copy(fractions.at[step], raw.at[step], small.at[2 + step]) for step in range(STEPS)
    ]
    for c in get_fractions:
        c.start()
    get_shifts.start()
    get_helm.start()

    zero = jnp.zeros((8, LANES), F32)

    def clear(base):
        for j in range(n_chunks):
            k = base + j
            north[k, 0:8] = zero
            north[k, 24:32] = zero
            for i in range(2):
                pot[i, k, 0:8] = zero
                pot[i, k, 40:48] = zero

    clear(0)
    pl.semaphore_wait(barrier, n_lon + 1)

    def in_refs(part, to_block, to_level, from_lon):
        if part < 4:
            return (fields.at[part, to_level, rows_of(to_block), :], x.at[part, :, cols_of(from_lon)])
        return (coded.at[part - 4, rows_of(to_block), :], frac.at[part - 4, :, cols_of(from_lon)])

    def send_part(part):
        def turn(j, _):
            peer = lax.rem(lon + j, n_lon)
            to_block, to_level = place_of(peer, lat, n_blocks)
            from_ref, to_ref = in_refs(part, to_block, to_level, lon)
            pltpu.make_async_remote_copy(
                src_ref=from_ref,
                dst_ref=to_ref,
                send_sem=in_send.at[part],
                recv_sem=in_recv.at[part],
                device_id={"lon": peer, "lat": lat},
                device_id_type=MESH,
            ).start()
            return 0

        lax.fori_loop(1, n_lon, turn, 0)
        from_ref, to_ref = in_refs(part, block, level, lon)
        pltpu.make_async_copy(from_ref, to_ref, in_recv.at[part]).start()

    def in_whole(part):
        return x.at[part] if part < 4 else frac.at[part - 4]

    def wait_in(part):
        whole = in_whole(part)
        pltpu.make_async_copy(whole, whole, in_recv.at[part]).wait()

    def wait_in_sent(part):
        sent = in_whole(part).at[:, 0 : n_cols - tile]
        pltpu.make_async_copy(sent, sent, in_send.at[part]).wait()

    def code(step):
        get_fractions[step].wait()
        coded[step] = ((raw[step] * UNITS + 0.5).astype(jnp.int32) - HALF).astype(jnp.int16)

    def decode(value):
        return value.astype(jnp.int32).astype(F32) * (1.0 / UNITS) + HALF / UNITS

    send_part(0)
    code(0)
    send_part(4)
    send_part(1)
    send_part(2)
    code(1)
    send_part(3)
    send_part(5)
    get_shifts.wait()
    get_helm.wait()

    lane16 = lax.broadcasted_iota(jnp.int32, (ROWS, LANES), 1)
    row8 = lax.broadcasted_iota(jnp.int32, (8, LANES), 0)

    def weight_of(start, rows):
        row = start + lax.broadcasted_iota(jnp.int32, (rows, LANES), 0)
        coef = jnp.full((rows, LANES), helm[level], F32)
        inverse = 1.0 / (1.0 + 4.0 * coef)
        inside = ((row >= ROWS) | has_above) & ((row < 2 * ROWS) | has_below)
        return jnp.where(inside, coef * inverse, 0.0), inverse

    def unpack(parts):
        def turn(base):
            for j in range(n_chunks):
                for f in parts:
                    field[f, base + j] = x[f, :, chunk(base + j)].astype(F32)

        turn(0)

    def advect(step, sources, targets):
        shift = shifts[step, block]
        taps = []
        for d in (1, 0, -1, -2):
            total = (shift + (n_cols - d)) & (n_cols - 1)
            taps.append((total // LANES, total & (LANES - 1)))
        from_here = [lane16 >= part for _, part in taps]

        def turn(base):
            weights = [cubic_weights(decode(frac[step, :, chunk(base + j)])) for j in range(n_chunks)]
            for f, to in zip(sources, targets):
                total = [None] * n_chunks
                for tap, (whole, part) in enumerate(taps):
                    before = None
                    for j in range(-1, n_chunks):
                        here = pltpu.roll(field[f, wrap(base + j - whole + n_chunks)], part, 1)
                        if j >= 0:
                            term = weights[j][tap] * jnp.where(from_here[tap], here, before)
                            total[j] = term if tap == 0 else total[j] + term
                        before = here
                for j in range(n_chunks):
                    to(base + j, total[j].astype(BF16))

        turn(0)

    def east_west(base, count, load):
        mid = load(base)
        ln = lax.broadcasted_iota(jnp.int32, mid.shape, 1)
        last, first = ln == LANES - 1, ln == 0
        before = pltpu.roll(load(wrap(base - 1 + n_chunks)), 1, 1)
        mid_east = pltpu.roll(mid, LANES - 1, 1)
        for j in range(count):
            after = load(wrap(base + j + 1))
            after_east = pltpu.roll(after, LANES - 1, 1)
            mid_west = pltpu.roll(mid, 1, 1)
            yield (
                base + j,
                mid,
                jnp.where(last, after_east, mid_east),
                jnp.where(first, before, mid_west),
            )
            mid, mid_east, before = after, after_east, mid_west

    def sources(step):
        def turn(base):
            for k, _, e, w in east_west(base, n_chunks, lambda k: adv[1, k]):
                own = adv[0, k] - 0.25 * ((e - w) + (north[k, 9:25] - north[k, 7:23]))
                src[k, ROWS : 2 * ROWS] = own
                top, bottom = own[0:8], own[8:16]
                with_last = jnp.where(row8 == 0, north[k, 23:31], top)
                with_first = jnp.where(row8 == 7, north[k, 1:9], bottom)
                down[step, k] = jnp.concatenate([with_last, bottom], axis=0).astype(BF16)
                up[step, k] = jnp.concatenate([top, with_first], axis=0).astype(BF16)

        turn(0)

    def halo_copies(step):
        return (
            pltpu.make_async_remote_copy(
                src_ref=down.at[step],
                dst_ref=above.at[step],
                send_sem=halo_send.at[step, 0],
                recv_sem=halo_recv.at[step, 0],
                device_id=dev_down,
                device_id_type=MESH,
            ),
            pltpu.make_async_remote_copy(
                src_ref=up.at[step],
                dst_ref=below.at[step],
                send_sem=halo_send.at[step, 1],
                recv_sem=halo_recv.at[step, 1],
                device_id=dev_up,
                device_id_type=MESH,
            ),
        )

    def complete(step):
        first_has, last_has = (row8 == 0) & has_below, (row8 == 7) & has_above

        def turn(base):
            for j in range(n_chunks):
                k = base + j
                a = jnp.where(has_above, above[step, k].astype(F32), 0.0)
                b = jnp.where(has_below, below[step, k].astype(F32), 0.0)
                src[k, 0:8] = a[0:8]
                src[k, 8:16] = a[8:16] - jnp.where(last_has, 0.25 * north[k, 1:9], 0.0)
                src[k, 16:24] = src[k, 16:24] + jnp.where(row8 == 0, 0.25 * a[0:8], 0.0)
                src[k, 24:32] = src[k, 24:32] - jnp.where(row8 == 7, 0.25 * b[8:16], 0.0)
                src[k, 32:40] = b[0:8] + jnp.where(first_has, 0.25 * north[k, 23:31], 0.0)
                src[k, 40:48] = b[8:16]

        turn(0)

    def first_sweep():
        weight, inverse = weight_of(8, 2 * ROWS)

        def turn(base):
            for k, mid, e, w in east_west(base, n_chunks, lambda k: src[k, 8:40]):
                fixed = mid * inverse
                scaled[k] = fixed
                pot[0, k, 8:40] = fixed + weight * ((e + w) + (src[k, 7:39] + src[k, 9:41]))

        turn(0)

    def later_sweeps():
        def sweep(now, start, weight):
            rows = weight.shape[0]
            for k, _, e, w in east_west(0, n_chunks, lambda k: pot[now, k, start : start + rows]):
                n = pot[now, k, start - 1 : start - 1 + rows]
                s = pot[now, k, start + 1 : start + 1 + rows]
                fixed = scaled[k, start - 8 : start - 8 + rows]
                pot[1 - now, k, start : start + rows] = fixed + weight * ((e + w) + (n + s))

        wide, _ = weight_of(8, 32)
        narrow, _ = weight_of(12, 24)

        def pair(i, _):
            sweep(0, 8, wide)
            sweep(1, 8, wide)
            return 0

        lax.fori_loop(0, 2, pair, 0)
        for i in range(4, SWEEPS - 1):
            sweep(i % 2, 12, narrow)

    solved = (SWEEPS - 1) % 2

    def update(base, count, to):
        for k, mid, e, w in east_west(base, count, lambda k: pot[solved, k, ROWS : 2 * ROWS]):
            n, s = pot[solved, k, ROWS - 1 : 2 * ROWS - 1], pot[solved, k, ROWS + 1 : 2 * ROWS + 1]
            to(0, k, mid.astype(BF16))
            to(1, k, (adv[1, k] - 0.25 * (e - w)).astype(BF16))
            to(2, k, (north[k, 8:24] - 0.25 * (s - n)).astype(BF16))

    def to_field(f, k, value):
        field[f, k] = value.astype(F32)

    def to_res(f, k, value):
        res[f, :, chunk(k)] = value

    def to_adv(f, k, value):
        if f == 2:
            north[k, 8:24] = value.astype(F32)
        else:
            adv[f, k] = value.astype(F32)

    def out_copy(part, peer):
        fs = slice(0, 3) if part == 0 else slice(3, 4)
        return pltpu.make_async_remote_copy(
            src_ref=res.at[fs, :, cols_of(peer)],
            dst_ref=out.at[fs, level, rows_of(block), :],
            send_sem=out_send.at[part],
            recv_sem=out_recv,
            device_id={"lon": peer, "lat": lat},
            device_id_type=MESH,
        )

    def out_keep(part):
        fs = slice(0, 3) if part == 0 else slice(3, 4)
        return pltpu.make_async_copy(
            res.at[fs, :, cols_of(lon)], out.at[fs, level, rows_of(block), :], out_recv
        )

    def update_and_send():
        per = tile // LANES

        def turn(j, _):
            peer = lax.rem(lon + j, n_lon)
            update(peer * per, per, to_res)

            @pl.when(j < n_lon)
            def _():
                out_copy(0, peer).start()

            return 0

        lax.fori_loop(1, n_lon + 1, turn, 0)
        out_keep(0).start()

    for step in range(STEPS):
        last = step == STEPS - 1
        if step == 0:
            wait_in(4)
            for f in range(3):
                wait_in(f)
                unpack((f,))
                advect(step, [f], [functools.partial(to_adv, f)])
        else:
            wait_in(5)
            advect(step, range(3), [functools.partial(to_adv, f) for f in range(3)])
        sources(step)
        copies = halo_copies(step)
        for c in copies:
            c.start()
        if step == 0:
            wait_in(3)
            unpack((3,))
        advect(step, [3 + step], [functools.partial(to_res if last else to_field, 3 + (not last))])
        if last:

            def send_res3(j, _):
                out_copy(1, lax.rem(lon + j, n_lon)).start()
                return 0

            lax.fori_loop(1, n_lon, send_res3, 0)
            out_keep(1).start()
        for c in copies:
            c.wait_recv()
        complete(step)
        first_sweep()
        later_sweeps()
        if last:
            update_and_send()
        else:
            update(0, n_chunks, to_field)

    for part in range(6):
        wait_in_sent(part)
    for step in range(STEPS):
        for c in halo_copies(step):
            c.wait_send()
    sent = res.at[0:3, :, 0 : n_cols - tile]
    pltpu.make_async_copy(sent, sent, out_send.at[0]).wait()
    sent = res.at[3:4, :, 0 : n_cols - tile]
    pltpu.make_async_copy(sent, sent, out_send.at[1]).wait()
    pltpu.make_async_copy(out, out, out_recv).wait()


def local(n_lon, n_lat, fields, shifts, fractions, helm_coef):
    n_cols = n_lon * fields.shape[3]
    n_chunks = n_cols // LANES
    return pl.pallas_call(
        functools.partial(kernel, n_lon, n_lat),
        out_shape=jax.ShapeDtypeStruct(fields.shape, BF16),
        in_specs=[pl.BlockSpec(memory_space=pltpu.HBM)] * 4,
        out_specs=pl.BlockSpec(memory_space=pl.ANY),
        scratch_shapes=[
            pltpu.SMEM(shifts.shape, jnp.int32),
            pltpu.SMEM(helm_coef.shape, F32),
            pltpu.VMEM(fractions.shape, F32),
            pltpu.VMEM(fractions.shape, jnp.int16),
            pltpu.VMEM((4, ROWS, n_cols), BF16),
            pltpu.VMEM((STEPS, ROWS, n_cols), jnp.int16),
            pltpu.VMEM((5, n_chunks, ROWS, LANES), F32),
            pltpu.VMEM((2, n_chunks, ROWS, LANES), F32),
            pltpu.VMEM((n_chunks, 2 * ROWS, LANES), F32),
            pltpu.VMEM((4, ROWS, n_cols), BF16),
            pltpu.VMEM((n_chunks, 3 * ROWS, LANES), F32),
            pltpu.VMEM((n_chunks, 2 * ROWS, LANES), F32),
            pltpu.VMEM((2, n_chunks, 3 * ROWS, LANES), F32),
            pltpu.VMEM((STEPS, n_chunks, ROWS, LANES), BF16),
            pltpu.VMEM((STEPS, n_chunks, ROWS, LANES), BF16),
            pltpu.VMEM((STEPS, n_chunks, ROWS, LANES), BF16),
            pltpu.VMEM((STEPS, n_chunks, ROWS, LANES), BF16),
            pltpu.SemaphoreType.DMA((2 + STEPS,)),
            pltpu.SemaphoreType.DMA((4 + STEPS,)),
            pltpu.SemaphoreType.DMA((4 + STEPS,)),
            pltpu.SemaphoreType.DMA((STEPS, 2)),
            pltpu.SemaphoreType.DMA((STEPS, 2)),
            pltpu.SemaphoreType.DMA((2,)),
            pltpu.SemaphoreType.DMA,
        ],
        compiler_params=pltpu.CompilerParams(
            collective_id=0, has_side_effects=True, vmem_limit_bytes=32 * 2**20
        ),
        name="transport",
    )(*[pltpu.with_memory_space_constraint(a, pltpu.HBM) for a in (fields, shifts, fractions, helm_coef)])


def solution(mesh):
    return jax.shard_map(
        functools.partial(local, mesh.shape["lon"], mesh.shape["lat"]),
        mesh=mesh,
        in_specs=(P(None, None, "lat", "lon"), P(None, "lat"), P(None, "lat", "lon"), P()),
        out_specs=P(None, None, "lat", "lon"),
        check_vma=False,
    )
```

```python
import functools

import jax
import jax.numpy as jnp
from jax import lax
from jax.experimental import pallas as pl
from jax.experimental.pallas import tpu as pltpu
from jax.sharding import PartitionSpec as P

STEPS = 2
SWEEPS = 8
ROWS = 16
LANES = 128
WAYS = 4
WINDOW = WAYS * LANES
F32 = jnp.float32
BF16 = jnp.bfloat16
UNITS, HALF = 65535.0, 32768
MESH = pl.DeviceIdType.MESH


def place_of(lon, lat, n_blocks):
    along = 2 * lax.div(lon, 4) + lax.rem(lon, 2)
    odd = lax.rem(lat, 2)
    return along + odd * (n_blocks - 1 - 2 * along), lax.rem(lax.div(lon, 2), 2)


def lon_of(block, level, lat, n_blocks):
    odd = lax.rem(lat, 2)
    along = block + odd * (n_blocks - 1 - 2 * block)
    return 4 * lax.div(along, 2) + 2 * level + lax.rem(along, 2)


def cubic_weights(a):
    am, ap, a2 = a - 1.0, a + 1.0, a - 2.0
    left, right = a * am, ap * a2
    return (
        left * a2 * (-1.0 / 6.0),
        right * am * 0.5,
        right * a * -0.5,
        ap * left * (1.0 / 6.0),
    )


def kernel(
    n_lon, n_lat, fields, shifts_hbm, fractions, helm_hbm, out,
    shifts, helm, raw, coded, deal, gather, x, frac, share, field, adv, north, res, src, scaled, pot, down, up, above, below,
    small, in_send, in_recv, halo_send, halo_recv, out_send, out_recv,
):
    n_cols = n_lon * fields.shape[3]
    tile = fields.shape[3]
    n_chunks = n_cols // LANES
    n_windows = n_cols // WINDOW
    n_blocks = fields.shape[2] // ROWS
    lon, lat = lax.axis_index("lon"), lax.axis_index("lat")
    block, level = place_of(lon, lat, n_blocks)

    prev_block = lax.rem(block + n_blocks - 1, n_blocks)
    next_block = lax.rem(block + 1, n_blocks)
    lat_up = lax.rem(lat + n_lat - (block == 0).astype(jnp.int32), n_lat)
    lat_down = lax.rem(lat + (block == n_blocks - 1).astype(jnp.int32), n_lat)
    dev_up = {"lon": lon_of(prev_block, level, lat_up, n_blocks), "lat": lat_up}
    dev_down = {"lon": lon_of(next_block, level, lat_down, n_blocks), "lat": lat_down}
    row_block = lat * n_blocks + block
    has_above = row_block > 0
    has_below = row_block < n_lat * n_blocks - 1

    def rows_of(b):
        return pl.ds(pl.multiple_of(b * ROWS, ROWS), ROWS)

    def cols_of(p):
        return pl.ds(pl.multiple_of(p * tile, tile), tile)

    def window(w):
        return pl.ds(pl.multiple_of(w * WINDOW, WINDOW), WINDOW)

    def wrap(w):
        return w & (n_windows - 1)

    barrier = pltpu.get_barrier_semaphore()

    def greet(j, _):
        peer = lax.rem(lon + j, n_lon)
        pl.semaphore_signal(barrier, inc=1, device_id={"lon": peer, "lat": lat}, device_id_type=MESH)
        return 0

    lax.fori_loop(1, n_lon, greet, 0)
    pl.semaphore_signal(barrier, inc=1, device_id=dev_up, device_id_type=MESH)
    pl.semaphore_signal(barrier, inc=1, device_id=dev_down, device_id_type=MESH)

    get_shifts = pltpu.make_async_copy(shifts_hbm, shifts, small.at[0])
    get_helm = pltpu.make_async_copy(helm_hbm, helm, small.at[1])
    get_fractions = [
        pltpu.make_async_copy(fractions.at[step], raw.at[step], small.at[2 + step]) for step in range(STEPS)
    ]
    for c in get_fractions:
        c.start()
    get_shifts.start()
    get_helm.start()

    row = lax.broadcasted_iota(jnp.int32, (WINDOW, WINDOW), 0)
    col = lax.broadcasted_iota(jnp.int32, (WINDOW, WINDOW), 1)
    deal[...] = jnp.where(row == WAYS * ((col & (LANES - 1))) + (col >> 7), 1.0, 0.0).astype(BF16)
    gather[...] = jnp.where(col == WAYS * ((row & (LANES - 1))) + (row >> 7), 1.0, 0.0).astype(BF16)

    zero = jnp.zeros((8, LANES), F32)

    def clear(base):
        for j in range(n_chunks):
            k = base + j
            north[k, 0:8] = zero
            north[k, 24:32] = zero
            for i in range(2):
                pot[i, k, 0:8] = zero
                pot[i, k, 40:48] = zero

    clear(0)
    pl.semaphore_wait(barrier, n_lon + 1)

    def in_refs(part, to_block, to_level, from_lon):
        if part < 4:
            return (fields.at[part, to_level, rows_of(to_block), :], x.at[part, :, cols_of(from_lon)])
        return (coded.at[part - 4, rows_of(to_block), :], frac.at[part - 4, :, cols_of(from_lon)])

    def send_part(part):
        def turn(j, _):
            peer = lax.rem(lon + j, n_lon)
            to_block, to_level = place_of(peer, lat, n_blocks)
            from_ref, to_ref = in_refs(part, to_block, to_level, lon)
            pltpu.make_async_remote_copy(
                src_ref=from_ref,
                dst_ref=to_ref,
                send_sem=in_send.at[part],
                recv_sem=in_recv.at[part],
                device_id={"lon": peer, "lat": lat},
                device_id_type=MESH,
            ).start()
            return 0

        lax.fori_loop(1, n_lon, turn, 0)
        from_ref, to_ref = in_refs(part, block, level, lon)
        pltpu.make_async_copy(from_ref, to_ref, in_recv.at[part]).start()

    def in_whole(part):
        return x.at[part] if part < 4 else frac.at[part - 4]

    def wait_in(part):
        whole = in_whole(part)
        pltpu.make_async_copy(whole, whole, in_recv.at[part]).wait()

    def wait_in_sent(part):
        sent = in_whole(part).at[:, 0 : n_cols - tile]
        pltpu.make_async_copy(sent, sent, in_send.at[part]).wait()

    def code(step):
        get_fractions[step].wait()
        coded[step] = ((raw[step] * UNITS + 0.5).astype(jnp.int32) - HALF).astype(jnp.int16)

    send_part(0)
    code(0)
    send_part(4)
    send_part(1)
    send_part(2)
    code(1)
    send_part(3)
    send_part(5)
    get_shifts.wait()
    get_helm.wait()

    lane16 = lax.broadcasted_iota(jnp.int32, (ROWS, LANES), 1)
    row8 = lax.broadcasted_iota(jnp.int32, (8, LANES), 0)

    def weight_of(start, rows):
        row = start + lax.broadcasted_iota(jnp.int32, (rows, LANES), 0)
        coef = jnp.full((rows, LANES), helm[level], F32)
        inverse = 1.0 / (1.0 + 4.0 * coef)
        inside = ((row >= ROWS) | has_above) & ((row < 2 * ROWS) | has_below)
        return jnp.where(inside, coef * inverse, 0.0), inverse

    def dealt(rows):
        return jnp.dot(jnp.concatenate(rows, axis=0), deal[...], preferred_element_type=F32)

    def natural(rows):
        return jnp.dot(jnp.concatenate(rows, axis=0), gather[...], preferred_element_type=F32)

    def piece(values, i, m):
        return values[i * ROWS : (i + 1) * ROWS, m * LANES : (m + 1) * LANES]

    def unpack(f):
        values = dealt([x[f, :, window(w)] for w in range(n_windows)])
        for w in range(n_windows):
            for m in range(WAYS):
                field[f, WAYS * w + m] = piece(values, w, m)

    def unpack_fractions(step):
        rows = [frac[step, :, window(w)].astype(jnp.int32) + HALF for w in range(n_windows)]
        high = dealt([(r >> 8).astype(F32).astype(BF16) for r in rows])
        low = dealt([(r & 255).astype(F32).astype(BF16) for r in rows])
        values = (high * 256.0 + low) * (1.0 / UNITS)
        for w in range(n_windows):
            for m in range(WAYS):
                share[step, WAYS * w + m] = piece(values, w, m)

    def advect(step, sources, targets):
        shift = shifts[step, block]
        taps = []
        for t in range(-2, WAYS + 1):
            back = (shift + (n_cols - t)) & (n_cols - 1)
            way = (n_cols - back) & (WAYS - 1)
            cells = (back + way) // WAYS
            taps.append((way, cells // LANES, cells & (LANES - 1)))
        from_here = [lane16 >= part for _, _, part in taps]

        def rolled(f, w, tap):
            way, whole, part = taps[tap]
            return pltpu.roll(field[f, WAYS * wrap(w - whole + 2 * n_windows) + way], part, 1)

        for f, to in zip(sources, targets):
            before = [rolled(f, -1, tap) for tap in range(len(taps))]
            for w in range(n_windows):
                here = [rolled(f, w, tap) for tap in range(len(taps))]
                values = [jnp.where(c, h, b) for c, h, b in zip(from_here, here, before)]
                before = here
                for m in range(WAYS):
                    k = WAYS * w + m
                    w0, w1, w2, w3 = cubic_weights(share[step, k])
                    total = w0 * values[m + 3] + w1 * values[m + 2] + w2 * values[m + 1] + w3 * values[m]
                    to(k, total.astype(BF16))

    def east_west(base, count, load):
        before = pltpu.roll(load(WAYS * wrap(base - 1 + n_windows) + WAYS - 1), 1, 1)
        start = load(WAYS * base)
        start_east = pltpu.roll(start, LANES - 1, 1)
        ln = lax.broadcasted_iota(jnp.int32, start.shape, 1)
        last, first = ln == LANES - 1, ln == 0
        for j in range(count):
            vals = [start] + [load(WAYS * (base + j) + m) for m in range(1, WAYS)]
            after = load(WAYS * wrap(base + j + 1))
            after_east = pltpu.roll(after, LANES - 1, 1)
            end_west = pltpu.roll(vals[-1], 1, 1)
            east = vals[1:] + [jnp.where(last, after_east, start_east)]
            west = [jnp.where(first, before, end_west)] + vals[:-1]
            for m in range(WAYS):
                yield WAYS * (base + j) + m, vals[m], east[m], west[m]
            start, start_east, before = after, after_east, end_west

    def sources(step):
        def turn(base):
            for k, _, e, w in east_west(base, n_windows, lambda k: adv[1, k]):
                own = adv[0, k] - 0.25 * ((e - w) + (north[k, 9:25] - north[k, 7:23]))
                src[k, ROWS : 2 * ROWS] = own
                top, bottom = own[0:8], own[8:16]
                with_last = jnp.where(row8 == 0, north[k, 23:31], top)
                with_first = jnp.where(row8 == 7, north[k, 1:9], bottom)
                down[step, k] = jnp.concatenate([with_last, bottom], axis=0).astype(BF16)
                up[step, k] = jnp.concatenate([top, with_first], axis=0).astype(BF16)

        turn(0)

    def halo_copies(step):
        return (
            pltpu.make_async_remote_copy(
                src_ref=down.at[step],
                dst_ref=above.at[step],
                send_sem=halo_send.at[step, 0],
                recv_sem=halo_recv.at[step, 0],
                device_id=dev_down,
                device_id_type=MESH,
            ),
            pltpu.make_async_remote_copy(
                src_ref=up.at[step],
                dst_ref=below.at[step],
                send_sem=halo_send.at[step, 1],
                recv_sem=halo_recv.at[step, 1],
                device_id=dev_up,
                device_id_type=MESH,
            ),
        )

    def complete(step):
        first_has, last_has = (row8 == 0) & has_below, (row8 == 7) & has_above

        def turn(base):
            for j in range(n_chunks):
                k = base + j
                a = jnp.where(has_above, above[step, k].astype(F32), 0.0)
                b = jnp.where(has_below, below[step, k].astype(F32), 0.0)
                src[k, 0:8] = a[0:8]
                src[k, 8:16] = a[8:16] - jnp.where(last_has, 0.25 * north[k, 1:9], 0.0)
                src[k, 16:24] = src[k, 16:24] + jnp.where(row8 == 0, 0.25 * a[0:8], 0.0)
                src[k, 24:32] = src[k, 24:32] - jnp.where(row8 == 7, 0.25 * b[8:16], 0.0)
                src[k, 32:40] = b[0:8] + jnp.where(first_has, 0.25 * north[k, 23:31], 0.0)
                src[k, 40:48] = b[8:16]

        turn(0)

    def first_sweep():
        weight, inverse = weight_of(8, 2 * ROWS)

        def turn(base):
            for k, mid, e, w in east_west(base, n_windows, lambda k: src[k, 8:40]):
                fixed = mid * inverse
                scaled[k] = fixed
                pot[0, k, 8:40] = fixed + weight * ((e + w) + (src[k, 7:39] + src[k, 9:41]))

        turn(0)

    def later_sweeps():
        def sweep(now, start, weight):
            rows = weight.shape[0]
            for k, _, e, w in east_west(0, n_windows, lambda k: pot[now, k, start : start + rows]):
                n = pot[now, k, start - 1 : start - 1 + rows]
                s = pot[now, k, start + 1 : start + 1 + rows]
                fixed = scaled[k, start - 8 : start - 8 + rows]
                pot[1 - now, k, start : start + rows] = fixed + weight * ((e + w) + (n + s))

        wide, _ = weight_of(8, 32)
        narrow, _ = weight_of(12, 24)

        def pair(i, _):
            sweep(0, 8, wide)
            sweep(1, 8, wide)
            return 0

        lax.fori_loop(0, 2, pair, 0)
        for i in range(4, SWEEPS - 1):
            sweep(i % 2, 12, narrow)

    solved = (SWEEPS - 1) % 2

    def update(base, count, to):
        for k, mid, e, w in east_west(base, count, lambda k: pot[solved, k, ROWS : 2 * ROWS]):
            n, s = pot[solved, k, ROWS - 1 : 2 * ROWS - 1], pot[solved, k, ROWS + 1 : 2 * ROWS + 1]
            to(0, k, mid.astype(BF16))
            to(1, k, (adv[1, k] - 0.25 * (e - w)).astype(BF16))
            to(2, k, (north[k, 8:24] - 0.25 * (s - n)).astype(BF16))

    def to_field(f, k, value):
        field[f, k] = value.astype(F32)

    def to_adv(f, k, value):
        if f == 2:
            north[k, 8:24] = value.astype(F32)
        else:
            adv[f, k] = value.astype(F32)

    def out_copy(part, peer):
        fs = slice(0, 3) if part == 0 else slice(3, 4)
        return pltpu.make_async_remote_copy(
            src_ref=res.at[fs, :, cols_of(peer)],
            dst_ref=out.at[fs, level, rows_of(block), :],
            send_sem=out_send.at[part],
            recv_sem=out_recv,
            device_id={"lon": peer, "lat": lat},
            device_id_type=MESH,
        )

    def out_keep(part):
        fs = slice(0, 3) if part == 0 else slice(3, 4)
        return pltpu.make_async_copy(
            res.at[fs, :, cols_of(lon)], out.at[fs, level, rows_of(block), :], out_recv
        )

    def update_and_send():
        per = WINDOW // tile
        core = lax.rem(lon, 2)

        def turn(j, _):
            w = wrap(lax.div(lon, per) + j + core * (n_windows - 2 * j))
            made = {}
            update(w, 1, lambda f, k, value: made.setdefault(f, []).append(value))
            rows = natural([jnp.concatenate(made[f], axis=1) for f in range(3)])
            for f in range(3):
                res[f, :, window(w)] = rows[f * ROWS : (f + 1) * ROWS].astype(BF16)
            for i in range(per):
                peer = per * w + i

                @pl.when(peer != lon)
                def _():
                    out_copy(0, peer).start()

            return 0

        lax.fori_loop(1, n_windows + 1, turn, 0)
        out_keep(0).start()

    def restore(f):
        chunks = [field[f, k].astype(BF16) for k in range(n_chunks)]
        rows = natural([jnp.concatenate(chunks[WAYS * w : WAYS * (w + 1)], axis=1) for w in range(n_windows)])
        for w in range(n_windows):
            res[f, :, window(w)] = rows[w * ROWS : (w + 1) * ROWS].astype(BF16)

    for step in range(STEPS):
        last = step == STEPS - 1
        if step == 0:
            wait_in(4)
            unpack_fractions(0)
            for f in range(3):
                wait_in(f)
                unpack(f)
                advect(step, [f], [functools.partial(to_adv, f)])
        else:
            advect(step, range(3), [functools.partial(to_adv, f) for f in range(3)])
        sources(step)
        copies = halo_copies(step)
        for c in copies:
            c.start()
        if step == 0:
            wait_in(3)
            unpack(3)
            wait_in(5)
            unpack_fractions(1)
        advect(step, [3 + step], [functools.partial(to_field, 4 - step)])
        if last:
            restore(3)

            def send_res3(j, _):
                out_copy(1, lax.rem(lon + j, n_lon)).start()
                return 0

            lax.fori_loop(1, n_lon, send_res3, 0)
            out_keep(1).start()
        for c in copies:
            c.wait_recv()
        complete(step)
        first_sweep()
        later_sweeps()
        if last:
            update_and_send()
        else:
            update(0, n_windows, to_field)

    for part in range(6):
        wait_in_sent(part)
    for step in range(STEPS):
        for c in halo_copies(step):
            c.wait_send()
    sent = res.at[0:3, :, 0 : n_cols - tile]
    pltpu.make_async_copy(sent, sent, out_send.at[0]).wait()
    sent = res.at[3:4, :, 0 : n_cols - tile]
    pltpu.make_async_copy(sent, sent, out_send.at[1]).wait()
    pltpu.make_async_copy(out, out, out_recv).wait()


def local(n_lon, n_lat, fields, shifts, fractions, helm_coef):
    n_cols = n_lon * fields.shape[3]
    n_chunks = n_cols // LANES
    return pl.pallas_call(
        functools.partial(kernel, n_lon, n_lat),
        out_shape=jax.ShapeDtypeStruct(fields.shape, BF16),
        in_specs=[pl.BlockSpec(memory_space=pltpu.HBM)] * 4,
        out_specs=pl.BlockSpec(memory_space=pl.ANY),
        scratch_shapes=[
            pltpu.SMEM(shifts.shape, jnp.int32),
            pltpu.SMEM(helm_coef.shape, F32),
            pltpu.VMEM(fractions.shape, F32),
            pltpu.VMEM(fractions.shape, jnp.int16),
            pltpu.VMEM((WINDOW, WINDOW), BF16),
            pltpu.VMEM((WINDOW, WINDOW), BF16),
            pltpu.VMEM((4, ROWS, n_cols), BF16),
            pltpu.VMEM((STEPS, ROWS, n_cols), jnp.int16),
            pltpu.VMEM((STEPS, n_chunks, ROWS, LANES), F32),
            pltpu.VMEM((5, n_chunks, ROWS, LANES), F32),
            pltpu.VMEM((2, n_chunks, ROWS, LANES), F32),
            pltpu.VMEM((n_chunks, 2 * ROWS, LANES), F32),
            pltpu.VMEM((4, ROWS, n_cols), BF16),
            pltpu.VMEM((n_chunks, 3 * ROWS, LANES), F32),
            pltpu.VMEM((n_chunks, 2 * ROWS, LANES), F32),
            pltpu.VMEM((2, n_chunks, 3 * ROWS, LANES), F32),
            pltpu.VMEM((STEPS, n_chunks, ROWS, LANES), BF16),
            pltpu.VMEM((STEPS, n_chunks, ROWS, LANES), BF16),
            pltpu.VMEM((STEPS, n_chunks, ROWS, LANES), BF16),
            pltpu.VMEM((STEPS, n_chunks, ROWS, LANES), BF16),
            pltpu.SemaphoreType.DMA((2 + STEPS,)),
            pltpu.SemaphoreType.DMA((4 + STEPS,)),
            pltpu.SemaphoreType.DMA((4 + STEPS,)),
            pltpu.SemaphoreType.DMA((STEPS, 2)),
            pltpu.SemaphoreType.DMA((STEPS, 2)),
            pltpu.SemaphoreType.DMA((2,)),
            pltpu.SemaphoreType.DMA,
        ],
        compiler_params=pltpu.CompilerParams(
            collective_id=0, has_side_effects=True, vmem_limit_bytes=32 * 2**20
        ),
        name="transport",
    )(*[pltpu.with_memory_space_constraint(a, pltpu.HBM) for a in (fields, shifts, fractions, helm_coef)])


def solution(mesh):
    return jax.shard_map(
        functools.partial(local, mesh.shape["lon"], mesh.shape["lat"]),
        mesh=mesh,
        in_specs=(P(None, None, "lat", "lon"), P(None, "lat"), P(None, "lat", "lon"), P()),
        out_specs=P(None, None, "lat", "lon"),
        check_vma=False,
    )
```

```python
import functools

import jax
import jax.numpy as jnp
from jax import lax
from jax.experimental import pallas as pl
from jax.experimental.pallas import tpu as pltpu
from jax.sharding import PartitionSpec as P

STEPS = 2
SWEEPS = 8
ROWS = 16
LANES = 128
WAYS = 4
WINDOW = WAYS * LANES
F32 = jnp.float32
BF16 = jnp.bfloat16
UNITS, HALF = 65535.0, 32768
MESH = pl.DeviceIdType.MESH


def place_of(lon, lat, n_blocks):
    along = 2 * lax.div(lon, 4) + lax.rem(lon, 2)
    odd = lax.rem(lat, 2)
    return along + odd * (n_blocks - 1 - 2 * along), lax.rem(lax.div(lon, 2), 2)


def lon_of(block, level, lat, n_blocks):
    odd = lax.rem(lat, 2)
    along = block + odd * (n_blocks - 1 - 2 * block)
    return 4 * lax.div(along, 2) + 2 * level + lax.rem(along, 2)


def cubic_weights(a):
    am, ap, a2 = a - 1.0, a + 1.0, a - 2.0
    left, right = a * am, ap * a2
    return (
        left * a2 * (-1.0 / 6.0),
        right * am * 0.5,
        right * a * -0.5,
        ap * left * (1.0 / 6.0),
    )


def kernel(
    n_lon, n_lat, fields, shifts_hbm, fractions, helm_hbm, out,
    shifts, helm, raw, coded, deal, gather, x, frac, share, field, adv, north, res, src, edge, scaled, pot, down, up, above, below,
    small, in_send, in_recv, halo_send, halo_recv, out_send, out_recv,
):
    n_cols = n_lon * fields.shape[3]
    tile = fields.shape[3]
    n_chunks = n_cols // LANES
    n_windows = n_cols // WINDOW
    n_blocks = fields.shape[2] // ROWS
    lon, lat = lax.axis_index("lon"), lax.axis_index("lat")
    block, level = place_of(lon, lat, n_blocks)

    prev_block = lax.rem(block + n_blocks - 1, n_blocks)
    next_block = lax.rem(block + 1, n_blocks)
    lat_up = lax.rem(lat + n_lat - (block == 0).astype(jnp.int32), n_lat)
    lat_down = lax.rem(lat + (block == n_blocks - 1).astype(jnp.int32), n_lat)
    dev_up = {"lon": lon_of(prev_block, level, lat_up, n_blocks), "lat": lat_up}
    dev_down = {"lon": lon_of(next_block, level, lat_down, n_blocks), "lat": lat_down}
    row_block = lat * n_blocks + block
    has_above = row_block > 0
    has_below = row_block < n_lat * n_blocks - 1

    def rows_of(b):
        return pl.ds(pl.multiple_of(b * ROWS, ROWS), ROWS)

    def cols_of(p):
        return pl.ds(pl.multiple_of(p * tile, tile), tile)

    def window(w):
        return pl.ds(pl.multiple_of(w * WINDOW, WINDOW), WINDOW)

    def wrap(w):
        return w & (n_windows - 1)

    barrier = pltpu.get_barrier_semaphore()

    def greet(j, _):
        peer = lax.rem(lon + j, n_lon)
        pl.semaphore_signal(barrier, inc=1, device_id={"lon": peer, "lat": lat}, device_id_type=MESH)
        return 0

    lax.fori_loop(1, n_lon, greet, 0)
    pl.semaphore_signal(barrier, inc=1, device_id=dev_up, device_id_type=MESH)
    pl.semaphore_signal(barrier, inc=1, device_id=dev_down, device_id_type=MESH)

    get_shifts = pltpu.make_async_copy(shifts_hbm, shifts, small.at[0])
    get_helm = pltpu.make_async_copy(helm_hbm, helm, small.at[1])
    get_fractions = [
        pltpu.make_async_copy(fractions.at[step], raw.at[step], small.at[2 + step]) for step in range(STEPS)
    ]
    for c in get_fractions:
        c.start()
    get_shifts.start()
    get_helm.start()

    row = lax.broadcasted_iota(jnp.int32, (WINDOW, WINDOW), 0)
    col = lax.broadcasted_iota(jnp.int32, (WINDOW, WINDOW), 1)
    deal[...] = jnp.where(row == WAYS * ((col & (LANES - 1))) + (col >> 7), 1.0, 0.0).astype(BF16)
    gather[...] = jnp.where(col == WAYS * ((row & (LANES - 1))) + (row >> 7), 1.0, 0.0).astype(BF16)

    zero = jnp.zeros((8, LANES), F32)

    def clear(base):
        for j in range(n_chunks):
            k = base + j
            north[k, 0:8] = zero
            north[k, 24:32] = zero
            for i in range(2):
                pot[i, k, 0:8] = zero
                pot[i, k, 40:48] = zero

    clear(0)
    pl.semaphore_wait(barrier, n_lon + 1)

    def in_refs(part, to_block, to_level, from_lon):
        if part < 4:
            return (fields.at[part, to_level, rows_of(to_block), :], x.at[part, :, cols_of(from_lon)])
        return (coded.at[part - 4, rows_of(to_block), :], frac.at[part - 4, :, cols_of(from_lon)])

    def send_part(part):
        def turn(j, _):
            peer = lax.rem(lon + j, n_lon)
            to_block, to_level = place_of(peer, lat, n_blocks)
            from_ref, to_ref = in_refs(part, to_block, to_level, lon)
            pltpu.make_async_remote_copy(
                src_ref=from_ref,
                dst_ref=to_ref,
                send_sem=in_send.at[part],
                recv_sem=in_recv.at[part],
                device_id={"lon": peer, "lat": lat},
                device_id_type=MESH,
            ).start()
            return 0

        lax.fori_loop(1, n_lon, turn, 0)
        from_ref, to_ref = in_refs(part, block, level, lon)
        pltpu.make_async_copy(from_ref, to_ref, in_recv.at[part]).start()

    def in_whole(part):
        return x.at[part] if part < 4 else frac.at[part - 4]

    def wait_in(part):
        whole = in_whole(part)
        pltpu.make_async_copy(whole, whole, in_recv.at[part]).wait()

    def wait_in_sent(part):
        sent = in_whole(part).at[:, 0 : n_cols - tile]
        pltpu.make_async_copy(sent, sent, in_send.at[part]).wait()

    def code(step):
        get_fractions[step].wait()
        coded[step] = ((raw[step] * UNITS + 0.5).astype(jnp.int32) - HALF).astype(jnp.int16)

    send_part(0)
    code(0)
    send_part(4)
    send_part(1)
    send_part(2)
    code(1)
    send_part(3)
    send_part(5)
    get_shifts.wait()
    get_helm.wait()

    lane16 = lax.broadcasted_iota(jnp.int32, (ROWS, LANES), 1)
    row8 = lax.broadcasted_iota(jnp.int32, (8, LANES), 0)

    def weight_of(start, rows):
        row = start + lax.broadcasted_iota(jnp.int32, (rows, LANES), 0)
        coef = jnp.full((rows, LANES), helm[level], F32)
        inverse = 1.0 / (1.0 + 4.0 * coef)
        inside = ((row >= ROWS) | has_above) & ((row < 2 * ROWS) | has_below)
        return jnp.where(inside, coef * inverse, 0.0), inverse

    def dealt(rows):
        return jnp.dot(jnp.concatenate(rows, axis=0), deal[...], preferred_element_type=F32)

    def natural(rows):
        return jnp.dot(jnp.concatenate(rows, axis=0), gather[...], preferred_element_type=F32)

    def piece(values, i, m):
        return values[i * ROWS : (i + 1) * ROWS, m * LANES : (m + 1) * LANES]

    def unpack(f):
        values = dealt([x[f, :, window(w)] for w in range(n_windows)])
        for w in range(n_windows):
            for m in range(WAYS):
                field[f, WAYS * w + m] = piece(values, w, m)

    def unpack_fractions(step):
        rows = [frac[step, :, window(w)].astype(jnp.int32) + HALF for w in range(n_windows)]
        high = dealt([(r >> 8).astype(F32).astype(BF16) for r in rows])
        low = dealt([(r & 255).astype(F32).astype(BF16) for r in rows])
        values = (high * 256.0 + low) * (1.0 / UNITS)
        for w in range(n_windows):
            for m in range(WAYS):
                share[step, WAYS * w + m] = piece(values, w, m)

    def advect(step, sources, targets):
        shift = shifts[step, block]
        taps = []
        for t in range(-2, WAYS + 1):
            back = (shift + (n_cols - t)) & (n_cols - 1)
            way = (n_cols - back) & (WAYS - 1)
            cells = (back + way) // WAYS
            taps.append((way, cells // LANES, cells & (LANES - 1)))
        from_here = [lane16 >= part for _, _, part in taps]

        def rolled(f, w, tap):
            way, whole, part = taps[tap]
            return pltpu.roll(field[f, WAYS * wrap(w - whole + 2 * n_windows) + way], part, 1)

        for f, to in zip(sources, targets):
            before = [rolled(f, -1, tap) for tap in range(len(taps))]
            for w in range(n_windows):
                here = [rolled(f, w, tap) for tap in range(len(taps))]
                values = [jnp.where(c, h, b) for c, h, b in zip(from_here, here, before)]
                before = here
                for m in range(WAYS):
                    k = WAYS * w + m
                    w0, w1, w2, w3 = cubic_weights(share[step, k])
                    total = w0 * values[m + 3] + w1 * values[m + 2] + w2 * values[m + 1] + w3 * values[m]
                    to(k, total.astype(BF16))

    def east_west(base, count, load):
        before = pltpu.roll(load(WAYS * wrap(base - 1 + n_windows) + WAYS - 1), 1, 1)
        start = load(WAYS * base)
        start_east = pltpu.roll(start, LANES - 1, 1)
        ln = lax.broadcasted_iota(jnp.int32, start.shape, 1)
        last, first = ln == LANES - 1, ln == 0
        for j in range(count):
            vals = [start] + [load(WAYS * (base + j) + m) for m in range(1, WAYS)]
            after = load(WAYS * wrap(base + j + 1))
            after_east = pltpu.roll(after, LANES - 1, 1)
            end_west = pltpu.roll(vals[-1], 1, 1)
            east = vals[1:] + [jnp.where(last, after_east, start_east)]
            west = [jnp.where(first, before, end_west)] + vals[:-1]
            for m in range(WAYS):
                yield WAYS * (base + j) + m, vals[m], east[m], west[m]
            start, start_east, before = after, after_east, end_west

    def sources(step):
        def turn(base):
            for k, _, e, w in east_west(base, n_windows, lambda k: adv[1, k]):
                own = adv[0, k] - 0.25 * ((e - w) + (north[k, 9:25] - north[k, 7:23]))
                src[k, ROWS : 2 * ROWS] = own
                down[step, k] = own[8:16].astype(BF16)
                up[step, k] = own[0:8].astype(BF16)
                edge[0, k : k + 1] = src[k, 23:24]
                edge[0, n_chunks + k : n_chunks + k + 1] = north[k, 23:24]
                edge[1, k : k + 1] = src[k, 24:25]
                edge[1, n_chunks + k : n_chunks + k + 1] = north[k, 8:9]

        turn(0)
        for i in range(n_chunks // 4):
            down[step, n_chunks + i] = edge[0, 8 * i : 8 * i + 8].astype(BF16)
            up[step, n_chunks + i] = edge[1, 8 * i : 8 * i + 8].astype(BF16)

    def halo_copies(step):
        return (
            pltpu.make_async_remote_copy(
                src_ref=down.at[step],
                dst_ref=above.at[step],
                send_sem=halo_send.at[step, 0],
                recv_sem=halo_recv.at[step, 0],
                device_id=dev_down,
                device_id_type=MESH,
            ),
            pltpu.make_async_remote_copy(
                src_ref=up.at[step],
                dst_ref=below.at[step],
                send_sem=halo_send.at[step, 1],
                recv_sem=halo_recv.at[step, 1],
                device_id=dev_up,
                device_id_type=MESH,
            ),
        )

    def complete(step):
        first_has, last_has = (row8 == 0) & has_below, (row8 == 7) & has_above
        for i in range(n_chunks // 4):
            a = above[step, n_chunks + i].astype(F32)
            b = below[step, n_chunks + i].astype(F32)
            edge[0, 8 * i : 8 * i + 8] = jnp.where(has_above, a, 0.0)
            edge[1, 8 * i : 8 * i + 8] = jnp.where(has_below, b, 0.0)
        for k in range(n_chunks):
            a = jnp.where(has_above, above[step, k].astype(F32), 0.0)
            b = jnp.where(has_below, below[step, k].astype(F32), 0.0)
            src[k, 8:16] = a - jnp.where(last_has, 0.25 * north[k, 1:9], 0.0)
            src[k, 32:40] = b + jnp.where(first_has, 0.25 * north[k, 23:31], 0.0)
            src[k, 7:8] = edge[0, k : k + 1]
            src[k, 40:41] = edge[1, k : k + 1]
            src[k, 16:17] = src[k, 16:17] + 0.25 * edge[0, n_chunks + k : n_chunks + k + 1]
            src[k, 31:32] = src[k, 31:32] - 0.25 * edge[1, n_chunks + k : n_chunks + k + 1]

    def first_sweep():
        weight, inverse = weight_of(8, 2 * ROWS)

        def turn(base):
            for k, mid, e, w in east_west(base, n_windows, lambda k: src[k, 8:40]):
                fixed = mid * inverse
                scaled[k] = fixed
                pot[0, k, 8:40] = fixed + weight * ((e + w) + (src[k, 7:39] + src[k, 9:41]))

        turn(0)

    def later_sweeps():
        def sweep(now, start, weight):
            rows = weight.shape[0]
            for k, _, e, w in east_west(0, n_windows, lambda k: pot[now, k, start : start + rows]):
                n = pot[now, k, start - 1 : start - 1 + rows]
                s = pot[now, k, start + 1 : start + 1 + rows]
                fixed = scaled[k, start - 8 : start - 8 + rows]
                pot[1 - now, k, start : start + rows] = fixed + weight * ((e + w) + (n + s))

        wide, _ = weight_of(8, 32)
        narrow, _ = weight_of(12, 24)

        def pair(i, _):
            sweep(0, 8, wide)
            sweep(1, 8, wide)
            return 0

        lax.fori_loop(0, 2, pair, 0)
        for i in range(4, SWEEPS - 1):
            sweep(i % 2, 12, narrow)

    solved = (SWEEPS - 1) % 2

    def update(base, count, to):
        for k, mid, e, w in east_west(base, count, lambda k: pot[solved, k, ROWS : 2 * ROWS]):
            n, s = pot[solved, k, ROWS - 1 : 2 * ROWS - 1], pot[solved, k, ROWS + 1 : 2 * ROWS + 1]
            to(0, k, mid.astype(BF16))
            to(1, k, (adv[1, k] - 0.25 * (e - w)).astype(BF16))
            to(2, k, (north[k, 8:24] - 0.25 * (s - n)).astype(BF16))

    def to_field(f, k, value):
        field[f, k] = value.astype(F32)

    def to_adv(f, k, value):
        if f == 2:
            north[k, 8:24] = value.astype(F32)
        else:
            adv[f, k] = value.astype(F32)

    def out_copy(part, peer):
        fs = slice(0, 3) if part == 0 else slice(3, 4)
        return pltpu.make_async_remote_copy(
            src_ref=res.at[fs, :, cols_of(peer)],
            dst_ref=out.at[fs, level, rows_of(block), :],
            send_sem=out_send.at[part],
            recv_sem=out_recv,
            device_id={"lon": peer, "lat": lat},
            device_id_type=MESH,
        )

    def out_keep(part):
        fs = slice(0, 3) if part == 0 else slice(3, 4)
        return pltpu.make_async_copy(
            res.at[fs, :, cols_of(lon)], out.at[fs, level, rows_of(block), :], out_recv
        )

    def update_and_send():
        per = WINDOW // tile
        core = lax.rem(lon, 2)

        def turn(j, _):
            w = wrap(lax.div(lon, per) + j + core * (n_windows - 2 * j))
            made = {}
            update(w, 1, lambda f, k, value: made.setdefault(f, []).append(value))
            rows = natural([jnp.concatenate(made[f], axis=1) for f in range(3)])
            for f in range(3):
                res[f, :, window(w)] = rows[f * ROWS : (f + 1) * ROWS].astype(BF16)
            for i in range(per):
                peer = per * w + i

                @pl.when(peer != lon)
                def _():
                    out_copy(0, peer).start()

            return 0

        lax.fori_loop(1, n_windows + 1, turn, 0)
        out_keep(0).start()

    def restore(f):
        chunks = [field[f, k].astype(BF16) for k in range(n_chunks)]
        rows = natural([jnp.concatenate(chunks[WAYS * w : WAYS * (w + 1)], axis=1) for w in range(n_windows)])
        for w in range(n_windows):
            res[f, :, window(w)] = rows[w * ROWS : (w + 1) * ROWS].astype(BF16)

    for step in range(STEPS):
        last = step == STEPS - 1
        if step == 0:
            wait_in(4)
            unpack_fractions(0)
            for f in range(3):
                wait_in(f)
                unpack(f)
                advect(step, [f], [functools.partial(to_adv, f)])
        else:
            advect(step, range(3), [functools.partial(to_adv, f) for f in range(3)])
        sources(step)
        copies = halo_copies(step)
        for c in copies:
            c.start()
        if step == 0:
            wait_in(3)
            unpack(3)
            wait_in(5)
            unpack_fractions(1)
        advect(step, [3 + step], [functools.partial(to_field, 4 - step)])
        if last:
            restore(3)

            def send_res3(j, _):
                out_copy(1, lax.rem(lon + j, n_lon)).start()
                return 0

            lax.fori_loop(1, n_lon, send_res3, 0)
            out_keep(1).start()
        for c in copies:
            c.wait_recv()
        complete(step)
        first_sweep()
        later_sweeps()
        if last:
            update_and_send()
        else:
            update(0, n_windows, to_field)

    for part in range(6):
        wait_in_sent(part)
    for step in range(STEPS):
        for c in halo_copies(step):
            c.wait_send()
    sent = res.at[0:3, :, 0 : n_cols - tile]
    pltpu.make_async_copy(sent, sent, out_send.at[0]).wait()
    sent = res.at[3:4, :, 0 : n_cols - tile]
    pltpu.make_async_copy(sent, sent, out_send.at[1]).wait()
    pltpu.make_async_copy(out, out, out_recv).wait()


def local(n_lon, n_lat, fields, shifts, fractions, helm_coef):
    n_cols = n_lon * fields.shape[3]
    n_chunks = n_cols // LANES
    return pl.pallas_call(
        functools.partial(kernel, n_lon, n_lat),
        out_shape=jax.ShapeDtypeStruct(fields.shape, BF16),
        in_specs=[pl.BlockSpec(memory_space=pltpu.HBM)] * 4,
        out_specs=pl.BlockSpec(memory_space=pl.ANY),
        scratch_shapes=[
            pltpu.SMEM(shifts.shape, jnp.int32),
            pltpu.SMEM(helm_coef.shape, F32),
            pltpu.VMEM(fractions.shape, F32),
            pltpu.VMEM(fractions.shape, jnp.int16),
            pltpu.VMEM((WINDOW, WINDOW), BF16),
            pltpu.VMEM((WINDOW, WINDOW), BF16),
            pltpu.VMEM((4, ROWS, n_cols), BF16),
            pltpu.VMEM((STEPS, ROWS, n_cols), jnp.int16),
            pltpu.VMEM((STEPS, n_chunks, ROWS, LANES), F32),
            pltpu.VMEM((5, n_chunks, ROWS, LANES), F32),
            pltpu.VMEM((2, n_chunks, ROWS, LANES), F32),
            pltpu.VMEM((n_chunks, 2 * ROWS, LANES), F32),
            pltpu.VMEM((4, ROWS, n_cols), BF16),
            pltpu.VMEM((n_chunks, 3 * ROWS, LANES), F32),
            pltpu.VMEM((2, 2 * n_chunks, LANES), F32),
            pltpu.VMEM((n_chunks, 2 * ROWS, LANES), F32),
            pltpu.VMEM((2, n_chunks, 3 * ROWS, LANES), F32),
            pltpu.VMEM((STEPS, n_chunks + n_chunks // 4, 8, LANES), BF16),
            pltpu.VMEM((STEPS, n_chunks + n_chunks // 4, 8, LANES), BF16),
            pltpu.VMEM((STEPS, n_chunks + n_chunks // 4, 8, LANES), BF16),
            pltpu.VMEM((STEPS, n_chunks + n_chunks // 4, 8, LANES), BF16),
            pltpu.SemaphoreType.DMA((2 + STEPS,)),
            pltpu.SemaphoreType.DMA((4 + STEPS,)),
            pltpu.SemaphoreType.DMA((4 + STEPS,)),
            pltpu.SemaphoreType.DMA((STEPS, 2)),
            pltpu.SemaphoreType.DMA((STEPS, 2)),
            pltpu.SemaphoreType.DMA((2,)),
            pltpu.SemaphoreType.DMA,
        ],
        compiler_params=pltpu.CompilerParams(
            collective_id=0, has_side_effects=True, vmem_limit_bytes=32 * 2**20
        ),
        name="transport",
    )(*[pltpu.with_memory_space_constraint(a, pltpu.HBM) for a in (fields, shifts, fractions, helm_coef)])


def solution(mesh):
    return jax.shard_map(
        functools.partial(local, mesh.shape["lon"], mesh.shape["lat"]),
        mesh=mesh,
        in_specs=(P(None, None, "lat", "lon"), P(None, "lat"), P(None, "lat", "lon"), P()),
        out_specs=P(None, None, "lat", "lon"),
        check_vma=False,
    )
```

```python
import functools

import jax
import jax.numpy as jnp
from jax import lax
from jax.experimental import pallas as pl
from jax.experimental.pallas import tpu as pltpu
from jax.sharding import PartitionSpec as P

STEPS = 2
SWEEPS = 8
ROWS = 16
LANES = 128
WAYS = 4
WINDOW = WAYS * LANES
F32 = jnp.float32
BF16 = jnp.bfloat16
UNITS, HALF = 65535.0, 32768
MESH = pl.DeviceIdType.MESH


def place_of(lon, lat, n_blocks):
    along = 2 * lax.div(lon, 4) + lax.rem(lon, 2)
    odd = lax.rem(lat, 2)
    return along + odd * (n_blocks - 1 - 2 * along), lax.rem(lax.div(lon, 2), 2)


def lon_of(block, level, lat, n_blocks):
    odd = lax.rem(lat, 2)
    along = block + odd * (n_blocks - 1 - 2 * block)
    return 4 * lax.div(along, 2) + 2 * level + lax.rem(along, 2)


def cubic_weights(a):
    am, ap, a2 = a - 1.0, a + 1.0, a - 2.0
    left, right = a * am, ap * a2
    return (
        left * a2 * (-1.0 / 6.0),
        right * am * 0.5,
        right * a * -0.5,
        ap * left * (1.0 / 6.0),
    )


def kernel(
    n_lon, n_lat, fields, shifts_hbm, fractions, helm_hbm, out,
    shifts, helm, raw, coded, deal, gather, x, frac, share, field, adv, north, res, src, edge, scaled, pot, down, up, above, below,
    small, in_send, in_recv, halo_send, halo_recv, out_send, out_recv,
):
    n_cols = n_lon * fields.shape[3]
    tile = fields.shape[3]
    n_chunks = n_cols // LANES
    n_windows = n_cols // WINDOW
    n_blocks = fields.shape[2] // ROWS
    lon, lat = lax.axis_index("lon"), lax.axis_index("lat")
    block, level = place_of(lon, lat, n_blocks)

    prev_block = lax.rem(block + n_blocks - 1, n_blocks)
    next_block = lax.rem(block + 1, n_blocks)
    lat_up = lax.rem(lat + n_lat - (block == 0).astype(jnp.int32), n_lat)
    lat_down = lax.rem(lat + (block == n_blocks - 1).astype(jnp.int32), n_lat)
    dev_up = {"lon": lon_of(prev_block, level, lat_up, n_blocks), "lat": lat_up}
    dev_down = {"lon": lon_of(next_block, level, lat_down, n_blocks), "lat": lat_down}
    row_block = lat * n_blocks + block
    has_above = row_block > 0
    has_below = row_block < n_lat * n_blocks - 1

    def rows_of(b):
        return pl.ds(pl.multiple_of(b * ROWS, ROWS), ROWS)

    def cols_of(p):
        return pl.ds(pl.multiple_of(p * tile, tile), tile)

    def window(w):
        return pl.ds(pl.multiple_of(w * WINDOW, WINDOW), WINDOW)

    def wrap(w):
        return w & (n_windows - 1)

    get_shifts = pltpu.make_async_copy(shifts_hbm, shifts, small.at[0])
    get_helm = pltpu.make_async_copy(helm_hbm, helm, small.at[1])
    get_fractions = [
        pltpu.make_async_copy(fractions.at[step], raw.at[step], small.at[2 + step]) for step in range(STEPS)
    ]
    for c in get_fractions:
        c.start()
    get_shifts.start()
    get_helm.start()

    barrier = pltpu.get_barrier_semaphore()

    def greet(j, _):
        peer = lax.rem(lon + j, n_lon)
        pl.semaphore_signal(barrier, inc=1, device_id={"lon": peer, "lat": lat}, device_id_type=MESH)
        return 0

    lax.fori_loop(1, n_lon, greet, 0, unroll=True)
    pl.semaphore_signal(barrier, inc=1, device_id=dev_up, device_id_type=MESH)
    pl.semaphore_signal(barrier, inc=1, device_id=dev_down, device_id_type=MESH)

    pl.semaphore_wait(barrier, n_lon + 1)

    def in_refs(part, to_block, to_level, from_lon):
        if part < 4:
            return (fields.at[part, to_level, rows_of(to_block), :], x.at[part, :, cols_of(from_lon)])
        return (coded.at[part - 4, rows_of(to_block), :], frac.at[part - 4, :, cols_of(from_lon)])

    def send_part(part):
        def turn(j, _):
            peer = lax.rem(lon + j, n_lon)
            to_block, to_level = place_of(peer, lat, n_blocks)
            from_ref, to_ref = in_refs(part, to_block, to_level, lon)
            pltpu.make_async_remote_copy(
                src_ref=from_ref,
                dst_ref=to_ref,
                send_sem=in_send.at[part],
                recv_sem=in_recv.at[part],
                device_id={"lon": peer, "lat": lat},
                device_id_type=MESH,
            ).start()
            return 0

        lax.fori_loop(1, n_lon, turn, 0, unroll=True)
        from_ref, to_ref = in_refs(part, block, level, lon)
        pltpu.make_async_copy(from_ref, to_ref, in_recv.at[part]).start()

    def in_whole(part):
        return x.at[part] if part < 4 else frac.at[part - 4]

    def wait_in(part):
        whole = in_whole(part)
        pltpu.make_async_copy(whole, whole, in_recv.at[part]).wait()

    def wait_in_sent(part):
        sent = in_whole(part).at[:, 0 : n_cols - tile]
        pltpu.make_async_copy(sent, sent, in_send.at[part]).wait()

    def code(step):
        get_fractions[step].wait()
        coded[step] = ((raw[step] * UNITS + 0.5).astype(jnp.int32) - HALF).astype(jnp.int16)

    send_part(0)
    code(0)
    send_part(4)
    send_part(1)
    send_part(2)
    code(1)
    send_part(3)
    send_part(5)
    row = lax.broadcasted_iota(jnp.int32, (WINDOW, WINDOW), 0)
    col = lax.broadcasted_iota(jnp.int32, (WINDOW, WINDOW), 1)
    deal[...] = jnp.where(row == WAYS * ((col & (LANES - 1))) + (col >> 7), 1.0, 0.0).astype(BF16)
    gather[...] = jnp.where(col == WAYS * ((row & (LANES - 1))) + (row >> 7), 1.0, 0.0).astype(BF16)

    zero = jnp.zeros((8, LANES), F32)

    def clear(base):
        for j in range(n_chunks):
            k = base + j
            north[k, 0:8] = zero
            north[k, 24:32] = zero
            for i in range(2):
                pot[i, k, 0:8] = zero
                pot[i, k, 40:48] = zero

    clear(0)
    get_shifts.wait()
    get_helm.wait()

    lane16 = lax.broadcasted_iota(jnp.int32, (ROWS, LANES), 1)
    row8 = lax.broadcasted_iota(jnp.int32, (8, LANES), 0)

    def weight_of(start, rows):
        row = start + lax.broadcasted_iota(jnp.int32, (rows, LANES), 0)
        coef = jnp.full((rows, LANES), helm[level], F32)
        inverse = 1.0 / (1.0 + 4.0 * coef)
        inside = ((row >= ROWS) | has_above) & ((row < 2 * ROWS) | has_below)
        return jnp.where(inside, coef * inverse, 0.0), inverse

    def dealt(rows):
        return jnp.dot(jnp.concatenate(rows, axis=0), deal[...], preferred_element_type=F32)

    def natural(rows):
        return jnp.dot(jnp.concatenate(rows, axis=0), gather[...], preferred_element_type=F32)

    def piece(values, i, m):
        return values[i * ROWS : (i + 1) * ROWS, m * LANES : (m + 1) * LANES]

    def unpack(f):
        values = dealt([x[f, :, window(w)] for w in range(n_windows)])
        for w in range(n_windows):
            for m in range(WAYS):
                field[f, WAYS * w + m] = piece(values, w, m)

    def unpack_fractions(step):
        rows = [frac[step, :, window(w)].astype(jnp.int32) + HALF for w in range(n_windows)]
        high = dealt([(r >> 8).astype(F32).astype(BF16) for r in rows])
        low = dealt([(r & 255).astype(F32).astype(BF16) for r in rows])
        values = (high * 256.0 + low) * (1.0 / UNITS)
        for w in range(n_windows):
            for m in range(WAYS):
                share[step, WAYS * w + m] = piece(values, w, m)

    def advect(step, sources, targets):
        shift = shifts[step, block]
        taps = []
        for t in range(-2, WAYS + 1):
            back = (shift + (n_cols - t)) & (n_cols - 1)
            way = (n_cols - back) & (WAYS - 1)
            cells = (back + way) // WAYS
            taps.append((way, cells // LANES, cells & (LANES - 1)))
        from_here = [lane16 >= part for _, _, part in taps]

        def rolled(f, w, tap):
            way, whole, part = taps[tap]
            return pltpu.roll(field[f, WAYS * wrap(w - whole + 2 * n_windows) + way], part, 1)

        for f, to in zip(sources, targets):
            before = [rolled(f, -1, tap) for tap in range(len(taps))]
            for w in range(n_windows):
                here = [rolled(f, w, tap) for tap in range(len(taps))]
                values = [jnp.where(c, h, b) for c, h, b in zip(from_here, here, before)]
                before = here
                for m in range(WAYS):
                    k = WAYS * w + m
                    w0, w1, w2, w3 = cubic_weights(share[step, k])
                    total = w0 * values[m + 3] + w1 * values[m + 2] + w2 * values[m + 1] + w3 * values[m]
                    to(k, total.astype(BF16))

    def east_west(base, count, load):
        before = pltpu.roll(load(WAYS * wrap(base - 1 + n_windows) + WAYS - 1), 1, 1)
        start = load(WAYS * base)
        start_east = pltpu.roll(start, LANES - 1, 1)
        ln = lax.broadcasted_iota(jnp.int32, start.shape, 1)
        last, first = ln == LANES - 1, ln == 0
        for j in range(count):
            vals = [start] + [load(WAYS * (base + j) + m) for m in range(1, WAYS)]
            after = load(WAYS * wrap(base + j + 1))
            after_east = pltpu.roll(after, LANES - 1, 1)
            end_west = pltpu.roll(vals[-1], 1, 1)
            east = vals[1:] + [jnp.where(last, after_east, start_east)]
            west = [jnp.where(first, before, end_west)] + vals[:-1]
            for m in range(WAYS):
                yield WAYS * (base + j) + m, vals[m], east[m], west[m]
            start, start_east, before = after, after_east, end_west

    def sources(step):
        def turn(base):
            for k, _, e, w in east_west(base, n_windows, lambda k: adv[1, k]):
                own = adv[0, k] - 0.25 * ((e - w) + (north[k, 9:25] - north[k, 7:23]))
                src[k, ROWS : 2 * ROWS] = own
                down[step, k] = own[8:16].astype(BF16)
                up[step, k] = own[0:8].astype(BF16)
                edge[0, k : k + 1] = src[k, 23:24]
                edge[0, n_chunks + k : n_chunks + k + 1] = north[k, 23:24]
                edge[1, k : k + 1] = src[k, 24:25]
                edge[1, n_chunks + k : n_chunks + k + 1] = north[k, 8:9]

        turn(0)
        for i in range(n_chunks // 4):
            down[step, n_chunks + i] = edge[0, 8 * i : 8 * i + 8].astype(BF16)
            up[step, n_chunks + i] = edge[1, 8 * i : 8 * i + 8].astype(BF16)

    def halo_copies(step):
        return (
            pltpu.make_async_remote_copy(
                src_ref=down.at[step],
                dst_ref=above.at[step],
                send_sem=halo_send.at[step, 0],
                recv_sem=halo_recv.at[step, 0],
                device_id=dev_down,
                device_id_type=MESH,
            ),
            pltpu.make_async_remote_copy(
                src_ref=up.at[step],
                dst_ref=below.at[step],
                send_sem=halo_send.at[step, 1],
                recv_sem=halo_recv.at[step, 1],
                device_id=dev_up,
                device_id_type=MESH,
            ),
        )

    def complete(step):
        first_has, last_has = (row8 == 0) & has_below, (row8 == 7) & has_above
        for i in range(n_chunks // 4):
            a = above[step, n_chunks + i].astype(F32)
            b = below[step, n_chunks + i].astype(F32)
            edge[0, 8 * i : 8 * i + 8] = jnp.where(has_above, a, 0.0)
            edge[1, 8 * i : 8 * i + 8] = jnp.where(has_below, b, 0.0)
        for k in range(n_chunks):
            a = jnp.where(has_above, above[step, k].astype(F32), 0.0)
            b = jnp.where(has_below, below[step, k].astype(F32), 0.0)
            src[k, 8:16] = a - jnp.where(last_has, 0.25 * north[k, 1:9], 0.0)
            src[k, 32:40] = b + jnp.where(first_has, 0.25 * north[k, 23:31], 0.0)
            src[k, 7:8] = edge[0, k : k + 1]
            src[k, 40:41] = edge[1, k : k + 1]
            src[k, 16:17] = src[k, 16:17] + 0.25 * edge[0, n_chunks + k : n_chunks + k + 1]
            src[k, 31:32] = src[k, 31:32] - 0.25 * edge[1, n_chunks + k : n_chunks + k + 1]

    def first_sweep():
        weight, inverse = weight_of(8, 2 * ROWS)

        def turn(base):
            for k, mid, e, w in east_west(base, n_windows, lambda k: src[k, 8:40]):
                fixed = mid * inverse
                scaled[k] = fixed
                pot[0, k, 8:40] = fixed + weight * ((e + w) + (src[k, 7:39] + src[k, 9:41]))

        turn(0)

    def later_sweeps():
        def sweep(now, start, weight):
            rows = weight.shape[0]
            for k, _, e, w in east_west(0, n_windows, lambda k: pot[now, k, start : start + rows]):
                n = pot[now, k, start - 1 : start - 1 + rows]
                s = pot[now, k, start + 1 : start + 1 + rows]
                fixed = scaled[k, start - 8 : start - 8 + rows]
                pot[1 - now, k, start : start + rows] = fixed + weight * ((e + w) + (n + s))

        wide, _ = weight_of(8, 32)
        narrow, _ = weight_of(12, 24)

        def pair(i, _):
            sweep(0, 8, wide)
            sweep(1, 8, wide)
            return 0

        lax.fori_loop(0, 2, pair, 0)
        for i in range(4, SWEEPS - 1):
            sweep(i % 2, 12, narrow)

    solved = (SWEEPS - 1) % 2

    def update(base, count, to):
        for k, mid, e, w in east_west(base, count, lambda k: pot[solved, k, ROWS : 2 * ROWS]):
            n, s = pot[solved, k, ROWS - 1 : 2 * ROWS - 1], pot[solved, k, ROWS + 1 : 2 * ROWS + 1]
            to(0, k, mid.astype(BF16))
            to(1, k, (adv[1, k] - 0.25 * (e - w)).astype(BF16))
            to(2, k, (north[k, 8:24] - 0.25 * (s - n)).astype(BF16))

    def to_field(f, k, value):
        field[f, k] = value.astype(F32)

    def to_adv(f, k, value):
        if f == 2:
            north[k, 8:24] = value.astype(F32)
        else:
            adv[f, k] = value.astype(F32)

    def out_copy(part, peer):
        fs = slice(0, 3) if part == 0 else slice(3, 4)
        return pltpu.make_async_remote_copy(
            src_ref=res.at[fs, :, cols_of(peer)],
            dst_ref=out.at[fs, level, rows_of(block), :],
            send_sem=out_send.at[part],
            recv_sem=out_recv,
            device_id={"lon": peer, "lat": lat},
            device_id_type=MESH,
        )

    def out_keep(part):
        fs = slice(0, 3) if part == 0 else slice(3, 4)
        return pltpu.make_async_copy(
            res.at[fs, :, cols_of(lon)], out.at[fs, level, rows_of(block), :], out_recv
        )

    def update_and_send():
        per = WINDOW // tile
        core = lax.rem(lon, 2)

        for j in range(1, n_windows + 1):
            w = wrap(lax.div(lon, per) + j + core * (n_windows - 2 * j))
            made = {}
            update(w, 1, lambda f, k, value: made.setdefault(f, []).append(value))
            rows = natural([jnp.concatenate(made[f], axis=1) for f in range(3)])
            for f in range(3):
                res[f, :, window(w)] = rows[f * ROWS : (f + 1) * ROWS].astype(BF16)
            if j < n_windows:
                for i in range(per):
                    out_copy(0, per * w + i).start()
            else:
                for i in range(1, per):
                    out_copy(0, per * w + lax.rem(lon + i, per)).start()
        out_keep(0).start()

    def restore(f):
        chunks = [field[f, k].astype(BF16) for k in range(n_chunks)]
        rows = natural([jnp.concatenate(chunks[WAYS * w : WAYS * (w + 1)], axis=1) for w in range(n_windows)])
        for w in range(n_windows):
            res[f, :, window(w)] = rows[w * ROWS : (w + 1) * ROWS].astype(BF16)

    for step in range(STEPS):
        last = step == STEPS - 1
        if step == 0:
            wait_in(4)
            unpack_fractions(0)
            for f in range(3):
                wait_in(f)
                unpack(f)
                advect(step, [f], [functools.partial(to_adv, f)])
        else:
            advect(step, range(3), [functools.partial(to_adv, f) for f in range(3)])
        sources(step)
        copies = halo_copies(step)
        for c in copies:
            c.start()
        if step == 0:
            wait_in(3)
            unpack(3)
            wait_in(5)
            unpack_fractions(1)
        advect(step, [3 + step], [functools.partial(to_field, 4 - step)])
        if last:
            restore(3)
        for c in copies:
            c.wait_recv()
        if last:
            def send_res3(j, _):
                out_copy(1, lax.rem(lon + j, n_lon)).start()
                return 0

            lax.fori_loop(1, n_lon, send_res3, 0, unroll=True)
            out_keep(1).start()
        complete(step)
        first_sweep()
        later_sweeps()
        if last:
            update_and_send()
        else:
            update(0, n_windows, to_field)

    for part in range(6):
        wait_in_sent(part)
    for step in range(STEPS):
        for c in halo_copies(step):
            c.wait_send()
    sent = res.at[0:3, :, 0 : n_cols - tile]
    pltpu.make_async_copy(sent, sent, out_send.at[0]).wait()
    sent = res.at[3:4, :, 0 : n_cols - tile]
    pltpu.make_async_copy(sent, sent, out_send.at[1]).wait()
    pltpu.make_async_copy(out, out, out_recv).wait()


def local(n_lon, n_lat, fields, shifts, fractions, helm_coef):
    n_cols = n_lon * fields.shape[3]
    n_chunks = n_cols // LANES
    return pl.pallas_call(
        functools.partial(kernel, n_lon, n_lat),
        out_shape=jax.ShapeDtypeStruct(fields.shape, BF16),
        in_specs=[pl.BlockSpec(memory_space=pltpu.HBM)] * 4,
        out_specs=pl.BlockSpec(memory_space=pl.ANY),
        scratch_shapes=[
            pltpu.SMEM(shifts.shape, jnp.int32),
            pltpu.SMEM(helm_coef.shape, F32),
            pltpu.VMEM(fractions.shape, F32),
            pltpu.VMEM(fractions.shape, jnp.int16),
            pltpu.VMEM((WINDOW, WINDOW), BF16),
            pltpu.VMEM((WINDOW, WINDOW), BF16),
            pltpu.VMEM((4, ROWS, n_cols), BF16),
            pltpu.VMEM((STEPS, ROWS, n_cols), jnp.int16),
            pltpu.VMEM((STEPS, n_chunks, ROWS, LANES), F32),
            pltpu.VMEM((5, n_chunks, ROWS, LANES), F32),
            pltpu.VMEM((2, n_chunks, ROWS, LANES), F32),
            pltpu.VMEM((n_chunks, 2 * ROWS, LANES), F32),
            pltpu.VMEM((4, ROWS, n_cols), BF16),
            pltpu.VMEM((n_chunks, 3 * ROWS, LANES), F32),
            pltpu.VMEM((2, 2 * n_chunks, LANES), F32),
            pltpu.VMEM((n_chunks, 2 * ROWS, LANES), F32),
            pltpu.VMEM((2, n_chunks, 3 * ROWS, LANES), F32),
            pltpu.VMEM((STEPS, n_chunks + n_chunks // 4, 8, LANES), BF16),
            pltpu.VMEM((STEPS, n_chunks + n_chunks // 4, 8, LANES), BF16),
            pltpu.VMEM((STEPS, n_chunks + n_chunks // 4, 8, LANES), BF16),
            pltpu.VMEM((STEPS, n_chunks + n_chunks // 4, 8, LANES), BF16),
            pltpu.SemaphoreType.DMA((2 + STEPS,)),
            pltpu.SemaphoreType.DMA((4 + STEPS,)),
            pltpu.SemaphoreType.DMA((4 + STEPS,)),
            pltpu.SemaphoreType.DMA((STEPS, 2)),
            pltpu.SemaphoreType.DMA((STEPS, 2)),
            pltpu.SemaphoreType.DMA((2,)),
            pltpu.SemaphoreType.DMA,
        ],
        compiler_params=pltpu.CompilerParams(
            collective_id=0, has_side_effects=True, vmem_limit_bytes=32 * 2**20
        ),
        name="transport",
    )(*[pltpu.with_memory_space_constraint(a, pltpu.HBM) for a in (fields, shifts, fractions, helm_coef)])


def solution(mesh):
    return jax.shard_map(
        functools.partial(local, mesh.shape["lon"], mesh.shape["lat"]),
        mesh=mesh,
        in_specs=(P(None, None, "lat", "lon"), P(None, "lat"), P(None, "lat", "lon"), P()),
        out_specs=P(None, None, "lat", "lon"),
        check_vma=False,
    )
```
